256 devices in a mesh: row: 8 (over z_hi, core), sa: 32 (over z_lo, x, y).
Axes of the slice: x: 4, y: 4, z: 8 (z_hi: 4, z_lo: 2; z = z_hi * 2 + z_lo), core: 2. Of those that a mesh axis runs over, the one named last changes fastest.
Arguments:
- rep_w1: float32 [16, 8, 128, 4096], P('row', None, None, 'sa'), may hold values from -6 to 6
- rep_w3: float32 [16, 8, 128, 4096], P('row', None, None, 'sa'), may hold values from -6 to 6
- rep_w2: float32 [16, 8, 128, 4096], P('row', None, None, 'sa'), may hold values from -6 to 6
- rep_gate: float32 [16, 8, 4096], P('row', None, 'sa'), may hold values from -6 to 6
Outputs:
- serve_w1: bfloat16 [8, 128, 4096], P('row', 'sa')
- serve_w3: bfloat16 [8, 128, 4096], P('row', 'sa')
- serve_w2: bfloat16 [8, 128, 4096], P('row', 'sa')
- serve_gate: bfloat16 [8, 4096], replicated
- soup_norms: float32 [8, 4], P('row')
- replica_norms: float32 [16, 8, 4], P('row')
The draws below stay inside these ranges and needn't reach their ends.
All inputs are finite; a program needn't handle non-finite values.
Results may differ from the reference program's by a relative error of at most 0.001.
Values may be sent and summed in bfloat16 or wider, within the bound.
No kernel may reach another device: no remote copies, remote signals or barrier semaphores. Data moves between devices by JAX's collectives and lax.ppermute only.
A program may use at most 64 MiB of HBM per device.

```python
import jax
import jax.numpy as jnp
from jax import lax

D = 4096
EXPERTS = 8
REPLICAS = 16
HID = 128


def raised(drawn, key, source, target, blocks, factor):
    def block_of(axis_at):
        return (jnp.arange(drawn.shape[axis_at]) // (drawn.shape[axis_at] // blocks)).reshape((-1,) + (1,) * (drawn.ndim - 1 - axis_at))

    first = jax.random.permutation(key, blocks)[block_of(target)]
    other_side = (block_of(target) + blocks // 2) % blocks
    return jnp.where((block_of(source) == first) | (block_of(source) == other_side), factor * drawn, drawn)


def block_scale(stream_key, shape, cuts, low, largest):
    def one(axis_at, blocks):
        draws = jax.random.uniform(jax.random.fold_in(jax.random.fold_in(stream_key, 6), axis_at), (blocks,), jnp.float32, low / len(cuts), largest / len(cuts))
        return jnp.repeat(jnp.exp(draws), shape[axis_at] // blocks).reshape((-1,) + (1,) * (len(shape) - axis_at - 1))

    factor_of = one(*cuts[0])
    for cut in cuts[1:]:
        factor_of = factor_of * one(*cut)
    return factor_of


def heavy_noise(own_key, dims, width, limit, shards, heavy, dtype=jnp.bfloat16):
    drawn = width * jax.random.normal(own_key, dims, jnp.float32)
    if shards:
        drawn = drawn * block_scale(own_key, dims, shards, -0.22, 0.18)
    return jnp.clip(raised(drawn, jax.random.fold_in(own_key, 3), *heavy), -limit, limit).astype(dtype)


def setup_inputs(seed: int = 0) -> dict:
    streams_of = jax.random.split(jax.random.key(seed), 5)
    rep_w1 = heavy_noise(streams_of[0], (REPLICAS, EXPERTS, HID, D), 1.0, 6.0, ((0, 8), (3, 32)), (3, 0, 16, 2.0), jnp.float32)
    rep_w3 = heavy_noise(streams_of[1], (REPLICAS, EXPERTS, HID, D), 1.0, 6.0, ((0, 8), (3, 32)), (3, 0, 16, 2.0), jnp.float32)
    rep_w2 = heavy_noise(streams_of[2], (REPLICAS, EXPERTS, HID, D), 1.0, 6.0, ((0, 8), (3, 32)), (3, 0, 16, 2.0), jnp.float32)
    rep_gate = heavy_noise(streams_of[3], (REPLICAS, EXPERTS, D), 1.0, 6.0, ((0, 8), (2, 32)), (2, 0, 16, 2.0), jnp.float32)
    return {"rep_w1": rep_w1, "rep_w3": rep_w3, "rep_w2": rep_w2, "rep_gate": rep_gate}


def square_sums(values, dims_summed):
    return lax.optimization_barrier(jnp.sum(values * values, axis=dims_summed))

def reference(rep_w1, rep_w3, rep_w2, rep_gate):
    weights = (rep_w1, rep_w3, rep_w2)
    served_list = []
    for weight in weights:
        soup = lax.optimization_barrier(jnp.sum(weight, axis=0)) / REPLICAS
        served_list.append(soup.astype(jnp.bfloat16))
    gate_soup = lax.optimization_barrier(jnp.sum(rep_gate, axis=0)) / REPLICAS
    serve_gate = gate_soup.astype(jnp.bfloat16)
    expert_entries = HID * D
    soup_columns = [jnp.sqrt(square_sums(served.astype(jnp.float32), (1, 2)) / expert_entries) for served in served_list]
    soup_columns.append(jnp.sqrt(square_sums(serve_gate.astype(jnp.float32), 1) / D))
    soup_norms = jnp.stack(soup_columns, axis=1)
    replica_columns = [jnp.sqrt(square_sums(weight, (2, 3)) / expert_entries) for weight in weights]
    replica_columns.append(jnp.sqrt(square_sums(rep_gate, 2) / D))
    replica_norms = jnp.stack(replica_columns, axis=2)
    return (served_list[0], served_list[1], served_list[2], serve_gate, soup_norms, replica_norms)
```

```python
import jax
import jax.numpy as jnp
from jax import lax
from jax.sharding import Mesh
from jax.sharding import PartitionSpec as P

ROW = ("zh", "c")
SA = ("zl", "x", "y")
SCALE = 2048.0


def halves(values, dtype):
    high = values.astype(dtype)
    low = (values - high.astype(jnp.float32)).astype(dtype)
    return high, low


def square_sums(values, dims_summed):
    return jnp.sum(values * values, axis=dims_summed)


def body(rep_w1, rep_w3, rep_w2, rep_gate):
    lines = lax.axis_size("zh")
    cores = lax.axis_size("c")
    peers = lax.axis_size(SA)
    replicas = rep_w1.shape[0] * lines * cores
    held, experts, hidden, width = rep_w1.shape
    model_width = width * peers
    core = lax.axis_index("c")
    line = lax.axis_index("zh")
    weights = (rep_w1, rep_w3, rep_w2)
    replica_parts = jnp.stack(
        [square_sums(weight, (2, 3)) for weight in weights] + [square_sums(rep_gate, 2)], axis=2
    )

    sums = [jnp.sum(weight, axis=0).reshape(lines, cores, hidden, width) for weight in weights]
    mine = jnp.concatenate([jnp.where(core == 0, s[:, 0], s[:, 1]) for s in sums], axis=1)
    others = jnp.concatenate([jnp.where(core == 0, s[:, 1], s[:, 0]) for s in sums], axis=1)
    gate = jnp.sum(rep_gate, axis=0)
    swap = [(0, 1), (1, 0)]
    sent = jnp.concatenate([others.reshape(-1, width), gate])
    came = lax.ppermute(sent, "c", swap)
    mine = mine + came[:-experts].reshape(mine.shape)
    gate = gate + came[-experts:]

    gate_halves = halves(gate * SCALE, jnp.float16)
    scaled = mine * SCALE
    pieces = [None] * lines
    for step in range(1, lines):
        to = lax.rem(line + step, lines)
        piece = lax.dynamic_index_in_dim(scaled, to, 0, keepdims=False).astype(jnp.float16)
        message = jnp.concatenate([piece, *gate_halves])
        pieces[step] = lax.ppermute(
            message, "zh", [(i, (i + step) % lines) for i in range(lines)]
        ).astype(jnp.float32)
    own = lax.dynamic_index_in_dim(scaled, line, 0, keepdims=False)
    rows = own.shape[0]
    soup = (own + pieces[2][:rows]) + (pieces[1][:rows] + pieces[3][:rows])
    gates = [gate_halves[0].astype(jnp.float32) + gate_halves[1].astype(jnp.float32)] + [
        piece[rows : rows + experts] + piece[rows + experts :] for piece in pieces[1:]
    ]
    gate_soup = (gates[0] + gates[2]) + (gates[1] + gates[3])
    served = (soup * (1.0 / (SCALE * replicas))).astype(jnp.bfloat16).reshape(3, hidden, width)
    serve_gate = (gate_soup * (1.0 / (SCALE * replicas))).astype(jnp.bfloat16)

    expert = line * cores + core
    gate_row = lax.dynamic_index_in_dim(serve_gate, expert, 0, keepdims=True)
    soup_parts = jnp.concatenate(
        [square_sums(served.astype(jnp.float32), (1, 2)), square_sums(gate_row.astype(jnp.float32), 1)]
    )
    parts = jnp.concatenate([replica_parts.reshape(-1), soup_parts])
    parts = jnp.pad(parts, (0, width - parts.shape[0])).reshape(1, width)
    small = jnp.concatenate([serve_gate, *halves(parts, jnp.bfloat16)])
    small = jnp.pad(small, ((0, -small.shape[0] % 4), (0, 0)))
    tiles = served.reshape(3, peers, hidden // peers, width).transpose(1, 0, 2, 3)
    tiles = tiles.reshape(peers, -1, width)
    message = jnp.concatenate([tiles, jnp.broadcast_to(small, (peers, *small.shape))], axis=1)
    arrived = lax.all_to_all(message, SA, 0, 0, tiled=True)
    each = hidden // peers
    outs = [
        arrived[:, k * each : (k + 1) * each].transpose(1, 0, 2).reshape(1, each, model_width)
        for k in range(3)
    ]
    whole_gate = arrived[:, 3 * each : 3 * each + experts].transpose(1, 0, 2).reshape(experts, model_width)
    ends = arrived[:, 3 * each + experts : 3 * each + experts + 2].astype(jnp.float32)
    totals = jnp.sum(ends, axis=(0, 1))
    counts = jnp.array([hidden * model_width] * 3 + [model_width], jnp.float32)
    n = held * experts * 4
    replica_norms = jnp.sqrt(totals[:n].reshape(held, experts, 4) / counts)
    soup_norms = jnp.sqrt(totals[n : n + 4].reshape(1, 4) / counts)
    return (*outs, whole_gate, soup_norms, replica_norms)


def solution(mesh):
    torus = Mesh(mesh.devices.reshape(mesh.shape["row"] // 2, 2, 2, 4, 4), ROW + SA)
    in_specs = (
        P(ROW, None, None, SA),
        P(ROW, None, None, SA),
        P(ROW, None, None, SA),
        P(ROW, None, SA),
    )
    out_specs = (
        P(ROW, SA, None),
        P(ROW, SA, None),
        P(ROW, SA, None),
        P(),
        P(ROW, None),
        P(ROW, None, None),
    )
    return jax.shard_map(body, mesh=torus, in_specs=in_specs, out_specs=out_specs, check_vma=False)
```

```python
import jax
import jax.numpy as jnp
from jax import lax
from jax.experimental import pallas as pl
from jax.experimental.pallas import tpu as pltpu
from jax.sharding import Mesh
from jax.sharding import PartitionSpec as P

ROW = ("zh", "c")
SA = ("zl", "x", "y")
SCALE = 2048.0


def halves(values, dtype):
    high = values.astype(dtype)
    low = (values - high.astype(jnp.float32)).astype(dtype)
    return high, low


def square_sums(values, dims_summed):
    return jnp.sum(values * values, axis=dims_summed)


def finish(arrived, out1, out3, out2, gate, soup, replica):
    peers, _, width = arrived.shape
    experts = gate.shape[0]
    each = out1.shape[1]
    for peer in range(peers):
        columns = pl.ds(peer * width, width)
        gate[:, columns] = arrived[peer, :experts, :]
        for k, out in enumerate((out1, out3, out2)):
            start = 2 * experts + k * each
            out[0, :, columns] = arrived[peer, start : start + each, :]
    sums = jnp.sum(arrived[:, experts : 2 * experts, :].astype(jnp.float32), axis=0)
    sums = sums + pltpu.roll(sums, width // 2, 1)
    over_rows = jnp.sum(sums, axis=0, keepdims=True)
    lane = lax.broadcasted_iota(jnp.int32, sums.shape, 1)
    column = jnp.where(lane < 2 * experts, lax.broadcasted_iota(jnp.int32, sums.shape, 0), lane)
    row_entries = peers * width
    entries = jnp.where(lax.rem(column, 4) == 3, row_entries, peers * each * row_entries)
    sums = jnp.where(lane < 2 * experts, sums, over_rows)
    norms = jnp.sqrt(sums / entries.astype(jnp.float32))
    replica[...] = norms[:, :experts]
    soup[...] = pltpu.roll(norms, width - 2 * experts, 1)[:1, :4]


def body(rep_w1, rep_w3, rep_w2, rep_gate):
    lines = lax.axis_size("zh")
    cores = lax.axis_size("c")
    peers = lax.axis_size(SA)
    replicas = rep_w1.shape[0] * lines * cores
    held, experts, hidden, width = rep_w1.shape
    each = hidden // peers
    model_width = width * peers
    core = lax.axis_index("c")
    line = lax.axis_index("zh")
    weights = (rep_w1, rep_w3, rep_w2)

    sums = [jnp.sum(weight, axis=0).reshape(lines, cores, hidden, width) for weight in weights]
    mine = jnp.concatenate([jnp.where(core == 0, s[:, 0], s[:, 1]) for s in sums], axis=1)
    others = jnp.concatenate([jnp.where(core == 0, s[:, 1], s[:, 0]) for s in sums], axis=1)
    gate = jnp.sum(rep_gate, axis=0)
    swap = [(0, 1), (1, 0)]
    sent = jnp.concatenate([others.reshape(-1, width), gate])
    came = lax.ppermute(sent, "c", swap)
    mine = mine + came[:-experts].reshape(mine.shape)
    gate = gate + came[-experts:]

    gate_halves = halves(gate * SCALE, jnp.float16)
    scaled = mine * SCALE
    pieces = [None] * lines
    for step in (2, 1, 3):
        to = lax.rem(line + step, lines)
        piece = lax.dynamic_index_in_dim(scaled, to, 0, keepdims=False).astype(jnp.float16)
        message = jnp.concatenate([piece, *gate_halves])
        pieces[step] = lax.ppermute(
            message, "zh", [(i, (i + step) % lines) for i in range(lines)]
        ).astype(jnp.float32)
    own = lax.dynamic_index_in_dim(scaled, line, 0, keepdims=False)
    rows = own.shape[0]
    soup = (own + pieces[2][:rows]) + (pieces[1][:rows] + pieces[3][:rows])
    gates = [gate_halves[0].astype(jnp.float32) + gate_halves[1].astype(jnp.float32)] + [
        piece[rows : rows + experts] + piece[rows + experts :] for piece in pieces[1:]
    ]
    gate_soup = (gates[0] + gates[2]) + (gates[1] + gates[3])
    served = (soup * (1.0 / (SCALE * replicas))).astype(jnp.bfloat16).reshape(3, hidden, width)
    serve_gate = (gate_soup * (1.0 / (SCALE * replicas))).astype(jnp.bfloat16)

    replica_parts = [square_sums(weight, (2, 3)) for weight in weights] + [square_sums(rep_gate, 2)]
    expert = line * cores + core
    served32, gate32 = served.astype(jnp.float32), serve_gate.astype(jnp.float32)
    own_row = lax.broadcasted_iota(jnp.int32, (experts, 1), 0) == expert
    own_gate = jnp.where(own_row, jnp.sum(gate32 * gate32, axis=1, keepdims=True), 0.0)
    soup_parts = jnp.sum(served32 * served32, axis=(1, 2)).reshape(1, 3)
    parts = jnp.stack(replica_parts, axis=1).reshape(held * 4, experts)
    parts = jnp.concatenate(
        [
            jnp.pad(parts, ((0, 0), (0, experts))),
            jnp.pad(soup_parts, ((0, experts - 1), (0, 0))),
            jnp.pad(own_gate, ((0, 0), (0, width // 2 - 2 * experts - 4))),
        ],
        axis=1,
    )
    small = jnp.concatenate(halves(parts, jnp.bfloat16), axis=1)
    small = jnp.broadcast_to(jnp.concatenate([serve_gate, small]), (peers, 2 * experts, width))
    tiles = served.reshape(3, peers, each, width).transpose(1, 0, 2, 3)
    tiles = tiles.reshape(peers, -1, width)
    message = jnp.concatenate([small, tiles, jnp.zeros((peers, each, width), jnp.bfloat16)], axis=1)
    arrived = lax.all_to_all(message, SA, 0, 0, tiled=True)
    shard = jax.ShapeDtypeStruct((1, each, model_width), jnp.bfloat16)
    *served_all, soup_norms, replica_norms = pl.pallas_call(
        finish,
        out_shape=(
            shard,
            shard,
            shard,
            jax.ShapeDtypeStruct((experts, model_width), jnp.bfloat16),
            jax.ShapeDtypeStruct((1, 4), jnp.float32),
            jax.ShapeDtypeStruct((held * 4, experts), jnp.float32),
        ),
        compiler_params=pltpu.CompilerParams(vmem_limit_bytes=4 << 20),
        name="finish",
    )(arrived)
    replica_norms = replica_norms.reshape(held, 4, experts).transpose(0, 2, 1)
    return (*served_all, soup_norms, replica_norms)


def solution(mesh):
    torus = Mesh(mesh.devices.reshape(mesh.shape["row"] // 2, 2, 2, 4, 4), ROW + SA)
    in_specs = (
        P(ROW, None, None, SA),
        P(ROW, None, None, SA),
        P(ROW, None, None, SA),
        P(ROW, None, SA),
    )
    out_specs = (
        P(ROW, SA, None),
        P(ROW, SA, None),
        P(ROW, SA, None),
        P(),
        P(ROW, None),
        P(ROW, None, None),
    )
    return jax.shard_map(body, mesh=torus, in_specs=in_specs, out_specs=out_specs, check_vma=False)
```

```python
import functools

import jax
import jax.numpy as jnp
from jax import lax
from jax.experimental import pallas as pl
from jax.experimental.pallas import tpu as pltpu
from jax.sharding import Mesh
from jax.sharding import PartitionSpec as P


ROW = ("zh", "c")
SA = ("zl", "x", "y")
SCALE = 2048.0
STEPS = (2, 1, 3)
ROOM = 6 << 20
F32 = jnp.float32


def call(kernel, out_shape, flops, scratch=(), in_hbm=0):
    def run(*args):
        specs = [pl.BlockSpec(memory_space=pltpu.HBM)] * in_hbm
        specs += [pl.BlockSpec(memory_space=pltpu.VMEM)] * (len(args) - in_hbm)
        return pl.pallas_call(
            kernel,
            out_shape=out_shape,
            in_specs=specs,
            out_specs=jax.tree.map(lambda _: pl.BlockSpec(memory_space=pltpu.VMEM), out_shape),
            scratch_shapes=scratch,
            compiler_params=pltpu.CompilerParams(vmem_limit_bytes=ROOM),
            cost_estimate=pl.CostEstimate(flops=flops, bytes_accessed=0, transcendentals=0),
        )(*args)

    return run


def array(shape, dtype=F32):
    return jax.ShapeDtypeStruct(shape, dtype)


def fold(values):
    rows, width = values.shape
    return jnp.sum((values * values).reshape(rows // 8, 8, width), axis=0)


def local(steps, lines, *refs):
    weights, refs = refs[:3], refs[3:]
    if len(steps) == 1:
        gate, sent, kept, parts, gate_parts, held, gate_held, done, gate_done = refs
    else:
        _, sent, kept, parts, held, done = refs
    line, core = lax.axis_index("zh"), lax.axis_index("c")
    hidden = held.shape[-2]
    copies = []
    for i, step in enumerate(steps):
        first = 2 * lax.rem(line + step, lines)
        for t, weight in enumerate(weights):
            source = weight.at[:, pl.ds(first, 2)]
            copies.append(pltpu.make_async_copy(source, held.at[i, t], done.at[i, t]))
    for copy in copies:
        copy.start()
    if len(steps) == 1:
        gate_copy = pltpu.make_async_copy(gate, gate_held, gate_done)
        gate_copy.start()
    for i in range(len(steps)):
        for t in range(3):
            copies[3 * i + t].wait()
            rows = pl.ds((3 * i + t) * hidden, hidden)
            sent[rows, :] = held[i, t, 0, 1 - core] + held[i, t, 1, 1 - core]
            kept[rows, :] = held[i, t, 0, core] + held[i, t, 1, core]
            for r in range(2):
                for e in range(2):
                    parts[i, r, t, e] = fold(held[i, t, r, e])
    if len(steps) == 1:
        gate_copy.wait()
        end = 3 * hidden * len(steps)
        sent[end : end + 8, :] = gate_held[0] + gate_held[1]
        gate_parts[...] = gate_held[...] * gate_held[...]


def prepare_first(kept, sent, came, message):
    rows = kept.shape[0]
    message[:rows, :] = (kept[...] + came[:rows, :]) * SCALE
    gate = (sent[rows:, :] + came[rows:, :]) * SCALE
    high = gate.astype(jnp.bfloat16).astype(F32)
    message[rows : rows + 8, :] = high
    message[rows + 8 :, :] = gate - high


def prepare_rest(kept, came, far, plus, minus, own):
    rows = own.shape[0]
    for i, message in enumerate((plus, minus)):
        part = pl.ds(i * rows, rows)
        message[:rows, :] = (kept[part, :] + came[part, :]) * SCALE
        message[rows:, :] = far[rows:, :]
    own[...] = (kept[2 * rows :, :] + came[2 * rows :, :]) * SCALE


def count(lines, far_parts, near_parts, gate_parts, small):
    line = lax.axis_index("zh")
    shape = small.shape
    lane = lax.broadcasted_iota(jnp.int32, shape, 1)
    row = lax.broadcasted_iota(jnp.int32, shape, 0)
    total = jnp.zeros(shape, F32)

    def put(total, value, where):
        return jnp.where(where, jnp.broadcast_to(value, shape), total)

    def whole(values):
        return jnp.sum(jnp.sum(values, axis=0, keepdims=True), axis=1, keepdims=True)

    for i, step in enumerate((*STEPS, 0)):
        part = far_parts.at[0] if i == 0 else near_parts.at[i - 1]
        expert = 2 * lax.rem(line + step, lines)
        for r in range(2):
            for t in range(3):
                for e in range(2):
                    total = put(total, whole(part[r, t, e]), (row == r * 4 + t) & (lane == expert + e))
    for r in range(2):
        gate_rows = jnp.sum(gate_parts[r], axis=1, keepdims=True)
        for e in range(8):
            total = put(total, gate_rows[e : e + 1, :], (row == r * 4 + 3) & (lane == e))
    small[...] = total


def combine(peers, lines, own, plus, far, minus, message, counted, out, held):
    line, core = lax.axis_index("zh"), lax.axis_index("c")
    rows, width = own.shape
    hidden = rows // 3
    each = hidden // peers
    factor = 1.0 / (SCALE * lines * 2 * 2)
    soup = (own[...] + far[:rows, :]) + (plus[:rows, :] + minus[:rows, :])
    held[...] = (soup * factor).astype(jnp.bfloat16).astype(F32)
    gates = [
        ref[rows : rows + 8, :] + ref[rows + 8 :, :]
        for ref in (message, far, plus, minus)
    ]
    serve_gate = (((gates[0] + gates[1]) + (gates[2] + gates[3])) * factor).astype(jnp.bfloat16)
    gate = serve_gate.astype(F32)

    lane = lax.broadcasted_iota(jnp.int32, (8, width), 1)
    row = lax.broadcasted_iota(jnp.int32, (8, width), 0)
    small = counted[...]
    for t in range(3):
        total = jnp.sum(fold(held[t * hidden : (t + 1) * hidden, :]), axis=0, keepdims=True)
        total = jnp.broadcast_to(jnp.sum(total, axis=1, keepdims=True), (8, width))
        small = jnp.where((row == 0) & (lane == 16 + t), total, small)
    squares = jnp.broadcast_to(jnp.sum(gate * gate, axis=1, keepdims=True), (8, width))
    small = jnp.where((row == line * 2 + core) & (lane == 19), squares, small)
    high = small.astype(jnp.bfloat16).astype(F32)
    small = (high + pltpu.roll(small - high, width // 2, 1)).astype(jnp.bfloat16)
    for peer in range(peers):
        out[peer, :8, :] = serve_gate
        out[peer, 8:16, :] = small
        for t in range(3):
            start = 16 + t * each
            source = t * hidden + peer * each
            out[peer, start : start + each, :] = held[source : source + each, :].astype(jnp.bfloat16)


def finish(arrived, out1, out3, out2, gate, soup, replica):
    peers, _, width = arrived.shape
    experts = gate.shape[0]
    each = out1.shape[1]
    for peer in range(peers):
        columns = pl.ds(peer * width, width)
        gate[:, columns] = arrived[peer, :experts, :]
        for k, out in enumerate((out1, out3, out2)):
            start = 2 * experts + k * each
            out[0, :, columns] = arrived[peer, start : start + each, :]
    sums = jnp.sum(arrived[:, experts : 2 * experts, :].astype(F32), axis=0)
    sums = sums + pltpu.roll(sums, width // 2, 1)
    over_rows = jnp.sum(sums, axis=0, keepdims=True)
    lane = lax.broadcasted_iota(jnp.int32, sums.shape, 1)
    column = jnp.where(lane < 2 * experts, lax.broadcasted_iota(jnp.int32, sums.shape, 0), lane)
    row_entries = peers * width
    entries = jnp.where(lax.rem(column, 4) == 3, row_entries, peers * each * row_entries)
    sums = jnp.where(lane < 2 * experts, sums, over_rows)
    norms = jnp.sqrt(sums / entries.astype(F32))
    replica[...] = norms[:, :experts]
    soup[...] = pltpu.roll(norms, width - 2 * experts, 1)[:1, :4]


def steps(rep_w1, rep_w3, rep_w2, rep_gate):
    lines = lax.axis_size("zh")
    peers = lax.axis_size(SA)
    held, experts, hidden, width = rep_w1.shape
    each = hidden // peers
    model_width = width * peers
    rows = 3 * hidden
    swap = [(0, 1), (1, 0)]
    rep_w1, rep_w3, rep_w2, rep_gate = (
        pltpu.with_memory_space_constraint(a, pltpu.HBM) for a in (rep_w1, rep_w3, rep_w2, rep_gate)
    )
    weights = (rep_w1, rep_w3, rep_w2)

    def buffers(n):
        return (pltpu.VMEM((n, 3, held, 2, hidden, width), F32),)

    far_sent, far_kept, far_parts, gate_parts = call(
        functools.partial(local, STEPS[:1], lines),
        (array((rows + 8, width)), array((rows, width)), array((1, held, 3, 2, 8, width)), array((held, 8, width))),
        1 << 22,
        buffers(1)
        + (pltpu.VMEM((held, 8, width), F32), pltpu.SemaphoreType.DMA((1, 3)), pltpu.SemaphoreType.DMA),
        in_hbm=4,
    )(*weights, rep_gate)
    far_came = lax.ppermute(far_sent, "c", swap)
    near_sent, near_kept, near_parts = call(
        functools.partial(local, (*STEPS[1:], 0), lines),
        (array((3 * rows, width)), array((3 * rows, width)), array((3, held, 3, 2, 8, width))),
        1 << 23,
        buffers(3) + (pltpu.SemaphoreType.DMA((3, 3)),),
        in_hbm=3,
    )(*weights, gate_parts)
    near_came = lax.ppermute(near_sent, "c", swap)

    def along(message, step):
        pairs = [(i, (i + step) % lines) for i in range(lines)]
        return lax.ppermute(message.astype(jnp.float16), "zh", pairs).astype(F32)

    half = array((rows + 16, width))
    far = call(prepare_first, half, 1 << 20)(far_kept, far_sent, far_came)
    came = {STEPS[0]: along(far, STEPS[0])}
    plus, minus, own = call(prepare_rest, (half, half, array((rows, width))), 1 << 21)(near_kept, near_came, far)
    came[STEPS[1]] = along(plus, STEPS[1])
    came[STEPS[2]] = along(minus, STEPS[2])
    counted = call(functools.partial(count, lines), array((8, width)), 1 << 20)(far_parts, near_parts, gate_parts)
    message = call(
        functools.partial(combine, peers, lines),
        array((peers, 32, width), jnp.bfloat16),
        1 << 22,
        (pltpu.VMEM((rows, width), F32),),
    )(own, came[1], came[2], came[3], far.astype(jnp.float16).astype(F32), counted)
    arrived = lax.all_to_all(message, SA, 0, 0, tiled=True)
    shard = array((1, each, model_width), jnp.bfloat16)
    *served, soup_norms, replica_norms = call(
        finish,
        (
            shard,
            shard,
            shard,
            array((experts, model_width), jnp.bfloat16),
            array((1, 4)),
            array((held * 4, experts)),
        ),
        1 << 20,
    )(arrived)
    replica_norms = replica_norms.reshape(held, 4, experts).transpose(0, 2, 1)
    return (*served, soup_norms, replica_norms)


def solution(mesh):
    torus = Mesh(mesh.devices.reshape(mesh.shape["row"] // 2, 2, 2, 4, 4), ROW + SA)
    in_specs = (
        P(ROW, None, None, SA),
        P(ROW, None, None, SA),
        P(ROW, None, None, SA),
        P(ROW, None, SA),
    )
    out_specs = (
        P(ROW, SA, None),
        P(ROW, SA, None),
        P(ROW, SA, None),
        P(),
        P(ROW, None),
        P(ROW, None, None),
    )
    return jax.shard_map(steps, mesh=torus, in_specs=in_specs, out_specs=out_specs, check_vma=False)
```

```python
import functools

import jax
import jax.numpy as jnp
from jax import lax
from jax.experimental import pallas as pl
from jax.experimental.pallas import tpu as pltpu
from jax.sharding import Mesh
from jax.sharding import PartitionSpec as P


ROW = ("zh", "c")
SA = ("zl", "x", "y")
SCALE = 2048.0
STEPS = (2, 1, 3)
ROOM = 6 << 20
F32 = jnp.float32


def call(kernel, out_shape, flops, scratch=(), in_hbm=0):
    def run(*args):
        specs = [pl.BlockSpec(memory_space=pltpu.HBM)] * in_hbm
        specs += [pl.BlockSpec(memory_space=pltpu.VMEM)] * (len(args) - in_hbm)
        return pl.pallas_call(
            kernel,
            out_shape=out_shape,
            in_specs=specs,
            out_specs=jax.tree.map(lambda _: pl.BlockSpec(memory_space=pltpu.VMEM), out_shape),
            scratch_shapes=scratch,
            compiler_params=pltpu.CompilerParams(vmem_limit_bytes=ROOM),
            cost_estimate=pl.CostEstimate(flops=flops, bytes_accessed=0, transcendentals=0),
        )(*args)

    return run


def array(shape, dtype=F32):
    return jax.ShapeDtypeStruct(shape, dtype)


def fold(values):
    rows, width = values.shape
    return jnp.sum((values * values).reshape(rows // 8, 8, width), axis=0)


def local(steps, lines, *refs):
    weights, refs = refs[:3], refs[3:]
    if steps == STEPS[:1]:
        gate, sent, kept, parts, gate_parts, held, gate_held, done, gate_done = refs
    else:
        _, sent, kept, parts, held, done = refs
    line, core = lax.axis_index("zh"), lax.axis_index("c")
    hidden = held.shape[-2]
    copies = []
    for i, step in enumerate(steps):
        first = 2 * lax.rem(line + step, lines)
        for t, weight in enumerate(weights):
            source = weight.at[:, pl.ds(first, 2)]
            copies.append(pltpu.make_async_copy(source, held.at[i, t], done.at[i, t]))
    for copy in copies:
        copy.start()
    if steps == STEPS[:1]:
        gate_copy = pltpu.make_async_copy(gate, gate_held, gate_done)
        gate_copy.start()
    for i in range(len(steps)):
        for t in range(3):
            copies[3 * i + t].wait()
            rows = pl.ds((3 * i + t) * hidden, hidden)
            sent[rows, :] = held[i, t, 0, 1 - core] + held[i, t, 1, 1 - core]
            kept[rows, :] = held[i, t, 0, core] + held[i, t, 1, core]
            for r in range(2):
                for e in range(2):
                    parts[i, r, t, e] = fold(held[i, t, r, e])
    if steps == STEPS[:1]:
        gate_copy.wait()
        end = 3 * hidden * len(steps)
        sent[end : end + 8, :] = gate_held[0] + gate_held[1]
        gate_parts[...] = gate_held[...] * gate_held[...]


def prepare_first(kept, sent, came, message):
    rows = kept.shape[0]
    message[:rows, :] = (kept[...] + came[:rows, :]) * SCALE
    gate = (sent[rows:, :] + came[rows:, :]) * SCALE
    high = gate.astype(jnp.bfloat16).astype(F32)
    message[rows : rows + 8, :] = high
    message[rows + 8 :, :] = gate - high


def prepare_rest(kept, came, far, plus, minus):
    rows = kept.shape[0] // 2
    for i, message in enumerate((plus, minus)):
        part = pl.ds(i * rows, rows)
        message[:rows, :] = (kept[part, :] + came[part, :]) * SCALE
        message[rows:, :] = far[rows:, :]


def count(lines, far_parts, near_parts, own_parts, gate_parts, small):
    line = lax.axis_index("zh")
    shape = small.shape
    lane = lax.broadcasted_iota(jnp.int32, shape, 1)
    row = lax.broadcasted_iota(jnp.int32, shape, 0)
    total = jnp.zeros(shape, F32)

    def put(total, value, where):
        return jnp.where(where, jnp.broadcast_to(value, shape), total)

    def whole(values):
        return jnp.sum(jnp.sum(values, axis=0, keepdims=True), axis=1, keepdims=True)

    for i, step in enumerate((*STEPS, 0)):
        part = (far_parts.at[0], near_parts.at[0], near_parts.at[1], own_parts.at[0])[i]
        expert = 2 * lax.rem(line + step, lines)
        for r in range(2):
            for t in range(3):
                for e in range(2):
                    total = put(total, whole(part[r, t, e]), (row == r * 4 + t) & (lane == expert + e))
    for r in range(2):
        gate_rows = jnp.sum(gate_parts[r], axis=1, keepdims=True)
        for e in range(8):
            total = put(total, gate_rows[e : e + 1, :], (row == r * 4 + 3) & (lane == e))
    small[...] = total


def combine(peers, lines, kept, other, plus, far, minus, message, counted, out, held):
    line, core = lax.axis_index("zh"), lax.axis_index("c")
    rows, width = kept.shape
    hidden = rows // 3
    each = hidden // peers
    factor = 1.0 / (SCALE * lines * 2 * 2)
    own = (kept[...] + other[...]) * SCALE
    soup = (own + far[:rows, :]) + (plus[:rows, :] + minus[:rows, :])
    held[...] = (soup * factor).astype(jnp.bfloat16).astype(F32)
    gates = [
        ref[rows : rows + 8, :] + ref[rows + 8 :, :]
        for ref in (message, far, plus, minus)
    ]
    serve_gate = (((gates[0] + gates[1]) + (gates[2] + gates[3])) * factor).astype(jnp.bfloat16)
    gate = serve_gate.astype(F32)

    lane = lax.broadcasted_iota(jnp.int32, (8, width), 1)
    row = lax.broadcasted_iota(jnp.int32, (8, width), 0)
    small = counted[...]
    for t in range(3):
        total = jnp.sum(fold(held[t * hidden : (t + 1) * hidden, :]), axis=0, keepdims=True)
        total = jnp.broadcast_to(jnp.sum(total, axis=1, keepdims=True), (8, width))
        small = jnp.where((row == 0) & (lane == 16 + t), total, small)
    squares = jnp.broadcast_to(jnp.sum(gate * gate, axis=1, keepdims=True), (8, width))
    small = jnp.where((row == line * 2 + core) & (lane == 19), squares, small)
    high = small.astype(jnp.bfloat16).astype(F32)
    small = (high + pltpu.roll(small - high, width // 2, 1)).astype(jnp.bfloat16)
    for peer in range(peers):
        out[peer, :8, :] = serve_gate
        out[peer, 8:16, :] = small
        for t in range(3):
            start = 16 + t * each
            source = t * hidden + peer * each
            out[peer, start : start + each, :] = held[source : source + each, :].astype(jnp.bfloat16)


def finish(arrived, out1, out3, out2, gate, soup, replica):
    peers, _, width = arrived.shape
    experts = gate.shape[0]
    each = out1.shape[1]
    for peer in range(peers):
        columns = pl.ds(peer * width, width)
        gate[:, columns] = arrived[peer, :experts, :]
        for k, out in enumerate((out1, out3, out2)):
            start = 2 * experts + k * each
            out[0, :, columns] = arrived[peer, start : start + each, :]
    sums = jnp.sum(arrived[:, experts : 2 * experts, :].astype(F32), axis=0)
    sums = sums + pltpu.roll(sums, width // 2, 1)
    over_rows = jnp.sum(sums, axis=0, keepdims=True)
    lane = lax.broadcasted_iota(jnp.int32, sums.shape, 1)
    column = jnp.where(lane < 2 * experts, lax.broadcasted_iota(jnp.int32, sums.shape, 0), lane)
    row_entries = peers * width
    entries = jnp.where(lax.rem(column, 4) == 3, row_entries, peers * each * row_entries)
    sums = jnp.where(lane < 2 * experts, sums, over_rows)
    norms = jnp.sqrt(sums / entries.astype(F32))
    replica[...] = norms[:, :experts]
    soup[...] = pltpu.roll(norms, width - 2 * experts, 1)[:1, :4]


def steps(rep_w1, rep_w3, rep_w2, rep_gate):
    lines = lax.axis_size("zh")
    peers = lax.axis_size(SA)
    held, experts, hidden, width = rep_w1.shape
    each = hidden // peers
    model_width = width * peers
    rows = 3 * hidden
    swap = [(0, 1), (1, 0)]
    rep_w1, rep_w3, rep_w2, rep_gate = (
        pltpu.with_memory_space_constraint(a, pltpu.HBM) for a in (rep_w1, rep_w3, rep_w2, rep_gate)
    )
    weights = (rep_w1, rep_w3, rep_w2)

    def buffers(n):
        return (pltpu.VMEM((n, 3, held, 2, hidden, width), F32),)

    far_sent, far_kept, far_parts, gate_parts = call(
        functools.partial(local, STEPS[:1], lines),
        (array((rows + 8, width)), array((rows, width)), array((1, held, 3, 2, 8, width)), array((held, 8, width))),
        1 << 22,
        buffers(1)
        + (pltpu.VMEM((held, 8, width), F32), pltpu.SemaphoreType.DMA((1, 3)), pltpu.SemaphoreType.DMA),
        in_hbm=4,
    )(*weights, rep_gate)
    far_came = lax.ppermute(far_sent, "c", swap)
    near_sent, near_kept, near_parts = call(
        functools.partial(local, STEPS[1:], lines),
        (array((2 * rows, width)), array((2 * rows, width)), array((2, held, 3, 2, 8, width))),
        1 << 23,
        buffers(2) + (pltpu.SemaphoreType.DMA((2, 3)),),
        in_hbm=3,
    )(*weights, gate_parts)
    near_came = lax.ppermute(near_sent, "c", swap)
    own_sent, own_kept, own_parts = call(
        functools.partial(local, (0,), lines),
        (array((rows, width)), array((rows, width)), array((1, held, 3, 2, 8, width))),
        1 << 22,
        buffers(1) + (pltpu.SemaphoreType.DMA((1, 3)),),
        in_hbm=3,
    )(*weights, gate_parts)
    own_came = lax.ppermute(own_sent, "c", swap)

    def along(message, step):
        pairs = [(i, (i + step) % lines) for i in range(lines)]
        return lax.ppermute(message.astype(jnp.float16), "zh", pairs).astype(F32)

    half = array((rows + 16, width))
    far = call(prepare_first, half, 1 << 20)(far_kept, far_sent, far_came)
    came = {STEPS[0]: along(far, STEPS[0])}
    plus, minus = call(prepare_rest, (half, half), 1 << 21)(
        near_kept, near_came, far
    )
    came[STEPS[1]] = along(plus, STEPS[1])
    came[STEPS[2]] = along(minus, STEPS[2])
    counted = call(functools.partial(count, lines), array((8, width)), 1 << 20)(
        far_parts, near_parts, own_parts, gate_parts
    )
    message = call(
        functools.partial(combine, peers, lines),
        array((peers, 32, width), jnp.bfloat16),
        1 << 22,
        (pltpu.VMEM((rows, width), F32),),
    )(own_kept, own_came, came[1], came[2], came[3], far.astype(jnp.float16).astype(F32), counted)
    arrived = lax.all_to_all(message, SA, 0, 0, tiled=True)
    shard = array((1, each, model_width), jnp.bfloat16)
    *served, soup_norms, replica_norms = call(
        finish,
        (
            shard,
            shard,
            shard,
            array((experts, model_width), jnp.bfloat16),
            array((1, 4)),
            array((held * 4, experts)),
        ),
        1 << 20,
    )(arrived)
    replica_norms = replica_norms.reshape(held, 4, experts).transpose(0, 2, 1)
    return (*served, soup_norms, replica_norms)


def solution(mesh):
    torus = Mesh(mesh.devices.reshape(mesh.shape["row"] // 2, 2, 2, 4, 4), ROW + SA)
    in_specs = (
        P(ROW, None, None, SA),
        P(ROW, None, None, SA),
        P(ROW, None, None, SA),
        P(ROW, None, SA),
    )
    out_specs = (
        P(ROW, SA, None),
        P(ROW, SA, None),
        P(ROW, SA, None),
        P(),
        P(ROW, None),
        P(ROW, None, None),
    )
    return jax.shard_map(steps, mesh=torus, in_specs=in_specs, out_specs=out_specs, check_vma=False)
```

```python
import functools

import jax
import jax.numpy as jnp
from jax import lax
from jax.experimental import pallas as pl
from jax.experimental.pallas import tpu as pltpu
from jax.sharding import Mesh
from jax.sharding import PartitionSpec as P


ROW = ("zh", "c")
SA = ("zl", "x", "y")
FULL = 32768.0
LEAST = 2.0**-100
TINY = 2.0**-30
STEPS = (2, 1, 3)
ROOM = 6 << 20
F32 = jnp.float32


def call(kernel, out_shape, flops, scratch=(), in_hbm=0):
    def run(*args):
        specs = [pl.BlockSpec(memory_space=pltpu.HBM)] * in_hbm
        specs += [pl.BlockSpec(memory_space=pltpu.VMEM)] * (len(args) - in_hbm)
        return pl.pallas_call(
            kernel,
            out_shape=out_shape,
            in_specs=specs,
            out_specs=jax.tree.map(lambda _: pl.BlockSpec(memory_space=pltpu.VMEM), out_shape),
            scratch_shapes=scratch,
            compiler_params=pltpu.CompilerParams(vmem_limit_bytes=ROOM),
            cost_estimate=pl.CostEstimate(flops=flops, bytes_accessed=0, transcendentals=0),
        )(*args)

    return run


def array(shape, dtype=F32):
    return jax.ShapeDtypeStruct(shape, dtype)


def fold(values):
    rows, width = values.shape
    return jnp.sum((values * values).reshape(rows // 8, 8, width), axis=0)


def local(steps, lines, *refs):
    weights, refs = refs[:3], refs[3:]
    if steps == STEPS[:1]:
        gate, sent, kept, parts, gate_parts, held, gate_held, done, gate_done = refs
    else:
        _, sent, kept, parts, held, done = refs
    line, core = lax.axis_index("zh"), lax.axis_index("c")
    hidden = held.shape[-2]
    copies = []
    for i, step in enumerate(steps):
        first = 2 * lax.rem(line + step, lines)
        for t, weight in enumerate(weights):
            source = weight.at[:, pl.ds(first, 2)]
            copies.append(pltpu.make_async_copy(source, held.at[i, t], done.at[i, t]))
    for copy in copies:
        copy.start()
    if steps == STEPS[:1]:
        gate_copy = pltpu.make_async_copy(gate, gate_held, gate_done)
        gate_copy.start()
    for i in range(len(steps)):
        for t in range(3):
            copies[3 * i + t].wait()
            rows = pl.ds((3 * i + t) * hidden, hidden)
            sent[rows, :] = held[i, t, 0, 1 - core] + held[i, t, 1, 1 - core]
            kept[rows, :] = held[i, t, 0, core] + held[i, t, 1, core]
            for r in range(2):
                for e in range(2):
                    parts[i, r, t, e] = fold(held[i, t, r, e])
    if steps == STEPS[:1]:
        gate_copy.wait()
        end = 3 * hidden * len(steps)
        sent[end : end + 8, :] = gate_held[0] + gate_held[1]
        gate_parts[...] = gate_held[...] * gate_held[...]


def encode(values):
    top = jnp.max(jnp.abs(values), axis=0, keepdims=True)
    power = jnp.ceil(jnp.log2(jnp.maximum(top, LEAST)))
    parts = values * jnp.exp2(-power)
    return parts * jnp.abs(parts) * FULL, power


def decode(codes, power):
    roots = codes * lax.rsqrt(jnp.maximum(jnp.abs(codes), TINY))
    return roots * (jnp.exp2(power) * (FULL**-0.5))


def write(message, blocks):
    powers = []
    rows = 0
    for block in blocks:
        codes, power = encode(block)
        message[rows : rows + block.shape[0], :] = codes
        rows += block.shape[0]
        powers.append(power)
    rest = jnp.zeros((8 - len(powers), powers[0].shape[1]), F32)
    message[rows:, :] = jnp.concatenate([*powers, rest])


def read(message, block):
    rows, _ = message.shape
    hidden = (rows - 16) // 3
    codes = message[rows - 16 : rows - 8, :] if block == 3 else message[block * hidden : (block + 1) * hidden, :]
    return decode(codes, message[rows - 8 + block : rows - 7 + block, :])


def prepare_first(kept, sent, came, message, gate):
    rows, _ = kept.shape
    hidden = rows // 3
    parts = [slice(t * hidden, (t + 1) * hidden) for t in range(3)]
    blocks = [kept[part, :] + came[part, :] for part in parts]
    gate[...] = sent[rows:, :] + came[rows:, :]
    write(message, [*blocks, sent[rows:, :] + came[rows:, :]])


def prepare_rest(kept, came, far, plus, minus):
    rows = kept.shape[0] // 2
    hidden = rows // 3
    for i, message in enumerate((plus, minus)):
        parts = [slice(i * rows + t * hidden, i * rows + (t + 1) * hidden) for t in range(3)]
        blocks = [kept[part, :] + came[part, :] for part in parts]
        write(message, blocks + [far[...]])


def count(lines, far_parts, near_parts, own_parts, gate_parts, small):
    line = lax.axis_index("zh")
    shape = small.shape
    lane = lax.broadcasted_iota(jnp.int32, shape, 1)
    row = lax.broadcasted_iota(jnp.int32, shape, 0)
    total = jnp.zeros(shape, F32)

    def put(total, value, where):
        return jnp.where(where, jnp.broadcast_to(value, shape), total)

    def whole(values):
        return jnp.sum(jnp.sum(values, axis=0, keepdims=True), axis=1, keepdims=True)

    for i, step in enumerate((*STEPS, 0)):
        part = (far_parts.at[0], near_parts.at[0], near_parts.at[1], own_parts.at[0])[i]
        expert = 2 * lax.rem(line + step, lines)
        for r in range(2):
            for t in range(3):
                for e in range(2):
                    total = put(total, whole(part[r, t, e]), (row == r * 4 + t) & (lane == expert + e))
    for r in range(2):
        gate_rows = jnp.sum(gate_parts[r], axis=1, keepdims=True)
        for e in range(8):
            total = put(total, gate_rows[e : e + 1, :], (row == r * 4 + 3) & (lane == e))
    small[...] = total


def combine(peers, lines, kept, other, plus, far, minus, message, counted, out, held):
    line, core = lax.axis_index("zh"), lax.axis_index("c")
    rows, width = kept.shape
    hidden = rows // 3
    each = hidden // peers
    factor = 1.0 / (lines * 2 * 2)
    for t in range(3):
        part = pl.ds(t * hidden, hidden)
        soup = kept[part, :] + other[part, :]
        soup = (soup + read(far, t)) + (read(plus, t) + read(minus, t))
        held[part, :] = (soup * factor).astype(jnp.bfloat16).astype(F32)
    gates = [read(ref, 3) for ref in (message, far, plus, minus)]
    serve_gate = (((gates[0] + gates[1]) + (gates[2] + gates[3])) * factor).astype(jnp.bfloat16)
    gate = serve_gate.astype(F32)

    lane = lax.broadcasted_iota(jnp.int32, (8, width), 1)
    row = lax.broadcasted_iota(jnp.int32, (8, width), 0)
    small = counted[...]
    for t in range(3):
        total = jnp.sum(fold(held[t * hidden : (t + 1) * hidden, :]), axis=0, keepdims=True)
        total = jnp.broadcast_to(jnp.sum(total, axis=1, keepdims=True), (8, width))
        small = jnp.where((row == 0) & (lane == 16 + t), total, small)
    squares = jnp.broadcast_to(jnp.sum(gate * gate, axis=1, keepdims=True), (8, width))
    small = jnp.where((row == line * 2 + core) & (lane == 19), squares, small)
    high = small.astype(jnp.bfloat16).astype(F32)
    small = (high + pltpu.roll(small - high, width // 2, 1)).astype(jnp.bfloat16)
    for peer in range(peers):
        out[peer, :8, :] = serve_gate
        out[peer, 8:16, :] = small
        for t in range(3):
            start = 16 + t * each
            source = t * hidden + peer * each
            out[peer, start : start + each, :] = held[source : source + each, :].astype(jnp.bfloat16)


def finish(arrived, out1, out3, out2, gate, soup, replica):
    peers, _, width = arrived.shape
    experts = gate.shape[0]
    each = out1.shape[1]
    for peer in range(peers):
        columns = pl.ds(peer * width, width)
        gate[:, columns] = arrived[peer, :experts, :]
        for k, out in enumerate((out1, out3, out2)):
            start = 2 * experts + k * each
            out[0, :, columns] = arrived[peer, start : start + each, :]
    sums = jnp.sum(arrived[:, experts : 2 * experts, :].astype(F32), axis=0)
    sums = sums + pltpu.roll(sums, width // 2, 1)
    over_rows = jnp.sum(sums, axis=0, keepdims=True)
    lane = lax.broadcasted_iota(jnp.int32, sums.shape, 1)
    column = jnp.where(lane < 2 * experts, lax.broadcasted_iota(jnp.int32, sums.shape, 0), lane)
    row_entries = peers * width
    entries = jnp.where(lax.rem(column, 4) == 3, row_entries, peers * each * row_entries)
    sums = jnp.where(lane < 2 * experts, sums, over_rows)
    norms = jnp.sqrt(sums / entries.astype(F32))
    replica[...] = norms[:, :experts]
    soup[...] = pltpu.roll(norms, width - 2 * experts, 1)[:1, :4]


def steps(rep_w1, rep_w3, rep_w2, rep_gate):
    lines = lax.axis_size("zh")
    peers = lax.axis_size(SA)
    held, experts, hidden, width = rep_w1.shape
    each = hidden // peers
    model_width = width * peers
    rows = 3 * hidden
    swap = [(0, 1), (1, 0)]
    rep_w1, rep_w3, rep_w2, rep_gate = (
        pltpu.with_memory_space_constraint(a, pltpu.HBM) for a in (rep_w1, rep_w3, rep_w2, rep_gate)
    )
    weights = (rep_w1, rep_w3, rep_w2)

    def buffers(n):
        return (pltpu.VMEM((n, 3, held, 2, hidden, width), F32),)

    far_sent, far_kept, far_parts, gate_parts = call(
        functools.partial(local, STEPS[:1], lines),
        (array((rows + 8, width)), array((rows, width)), array((1, held, 3, 2, 8, width)), array((held, 8, width))),
        1 << 22,
        buffers(1)
        + (pltpu.VMEM((held, 8, width), F32), pltpu.SemaphoreType.DMA((1, 3)), pltpu.SemaphoreType.DMA),
        in_hbm=4,
    )(*weights, rep_gate)
    far_came = lax.ppermute(far_sent, "c", swap)
    near_sent, near_kept, near_parts = call(
        functools.partial(local, STEPS[1:], lines),
        (array((2 * rows, width)), array((2 * rows, width)), array((2, held, 3, 2, 8, width))),
        1 << 23,
        buffers(2) + (pltpu.SemaphoreType.DMA((2, 3)),),
        in_hbm=3,
    )(*weights, gate_parts)
    near_came = lax.ppermute(near_sent, "c", swap)
    own_sent, own_kept, own_parts = call(
        functools.partial(local, (0,), lines),
        (array((rows, width)), array((rows, width)), array((1, held, 3, 2, 8, width))),
        1 << 22,
        buffers(1) + (pltpu.SemaphoreType.DMA((1, 3)),),
        in_hbm=3,
    )(*weights, gate_parts)
    own_came = lax.ppermute(own_sent, "c", swap)

    def along(message, step):
        pairs = [(i, (i + step) % lines) for i in range(lines)]
        return lax.ppermute(message.astype(jnp.float16), "zh", pairs).astype(F32)

    half = array((rows + 16, width))
    far, gate = call(prepare_first, (half, array((8, width))), 1 << 20)(far_kept, far_sent, far_came)
    came = {STEPS[0]: along(far, STEPS[0])}
    plus, minus = call(prepare_rest, (half, half), 1 << 21)(
        near_kept, near_came, gate
    )
    came[STEPS[1]] = along(plus, STEPS[1])
    came[STEPS[2]] = along(minus, STEPS[2])
    counted = call(functools.partial(count, lines), array((8, width)), 1 << 20)(
        far_parts, near_parts, own_parts, gate_parts
    )
    message = call(
        functools.partial(combine, peers, lines),
        array((peers, 32, width), jnp.bfloat16),
        1 << 22,
        (pltpu.VMEM((rows, width), F32),),
    )(own_kept, own_came, came[1], came[2], came[3], far.astype(jnp.float16).astype(F32), counted)
    arrived = lax.all_to_all(message, SA, 0, 0, tiled=True)
    shard = array((1, each, model_width), jnp.bfloat16)
    *served, soup_norms, replica_norms = call(
        finish,
        (
            shard,
            shard,
            shard,
            array((experts, model_width), jnp.bfloat16),
            array((1, 4)),
            array((held * 4, experts)),
        ),
        1 << 20,
    )(arrived)
    replica_norms = replica_norms.reshape(held, 4, experts).transpose(0, 2, 1)
    return (*served, soup_norms, replica_norms)


def solution(mesh):
    torus = Mesh(mesh.devices.reshape(mesh.shape["row"] // 2, 2, 2, 4, 4), ROW + SA)
    in_specs = (
        P(ROW, None, None, SA),
        P(ROW, None, None, SA),
        P(ROW, None, None, SA),
        P(ROW, None, SA),
    )
    out_specs = (
        P(ROW, SA, None),
        P(ROW, SA, None),
        P(ROW, SA, None),
        P(),
        P(ROW, None),
        P(ROW, None, None),
    )
    return jax.shard_map(steps, mesh=torus, in_specs=in_specs, out_specs=out_specs, check_vma=False)
```

```python
import functools

import jax
import jax.numpy as jnp
from jax import lax
from jax.experimental import pallas as pl
from jax.experimental.pallas import tpu as pltpu
from jax.sharding import Mesh
from jax.sharding import PartitionSpec as P


ROW = ("zh", "c")
SA = ("zl", "x", "y")
FULL = 32768.0
LEAST = 2.0**-100
TINY = 2.0**-30
STEPS = (2, 1, 3)
ROOM = 6 << 20
F32 = jnp.float32


def call(kernel, out_shape, flops, scratch=(), in_hbm=0):
    def run(*args):
        specs = [pl.BlockSpec(memory_space=pltpu.HBM)] * in_hbm
        specs += [pl.BlockSpec(memory_space=pltpu.VMEM)] * (len(args) - in_hbm)
        return pl.pallas_call(
            kernel,
            out_shape=out_shape,
            in_specs=specs,
            out_specs=jax.tree.map(lambda _: pl.BlockSpec(memory_space=pltpu.VMEM), out_shape),
            scratch_shapes=scratch,
            compiler_params=pltpu.CompilerParams(vmem_limit_bytes=ROOM),
            cost_estimate=pl.CostEstimate(flops=flops, bytes_accessed=0, transcendentals=0),
        )(*args)

    return run


def array(shape, dtype=F32):
    return jax.ShapeDtypeStruct(shape, dtype)


def fold(values):
    rows, width = values.shape
    return jnp.sum((values * values).reshape(rows // 8, 8, width), axis=0)


def local(steps, lines, *refs):
    weights, refs = refs[:3], refs[3:]
    if steps == STEPS[:1]:
        gate, sent, kept, parts, gate_parts, held, gate_held, done, gate_done = refs
    else:
        _, sent, kept, parts, held, done = refs
    line, core = lax.axis_index("zh"), lax.axis_index("c")
    hidden = held.shape[-2]
    copies = []
    for i, step in enumerate(steps):
        first = 2 * lax.rem(line + step, lines)
        for t, weight in enumerate(weights):
            source = weight.at[:, pl.ds(first, 2)]
            copies.append(pltpu.make_async_copy(source, held.at[i, t], done.at[i, t]))
    if steps == STEPS[:1]:
        gate_copy = pltpu.make_async_copy(gate, gate_held, gate_done)
        gate_copy.start()
    for copy in copies:
        copy.start()
    for i in range(len(steps)):
        for t in range(3):
            copies[3 * i + t].wait()
            rows = pl.ds((3 * i + t) * hidden, hidden)
            sent[rows, :] = held[i, t, 0, 1 - core] + held[i, t, 1, 1 - core]
            kept[rows, :] = held[i, t, 0, core] + held[i, t, 1, core]
            for r in range(2):
                for e in range(2):
                    parts[i, r, t, e] = fold(held[i, t, r, e])
    if steps == STEPS[:1]:
        gate_copy.wait()
        end = 3 * hidden * len(steps)
        sent[end : end + 8, :] = gate_held[0] + gate_held[1]
        gate_parts[...] = gate_held[...] * gate_held[...]


def encode(values):
    top = jnp.max(jnp.abs(values), axis=0, keepdims=True)
    power = jnp.ceil(jnp.log2(jnp.maximum(top, LEAST)))
    parts = values * jnp.exp2(-power)
    return parts * jnp.abs(parts) * FULL, power


def decode(codes, power):
    roots = codes * lax.rsqrt(jnp.maximum(jnp.abs(codes), TINY))
    return roots * (jnp.exp2(power) * (FULL**-0.5))


def write(message, blocks):
    powers = []
    rows = 0
    for block in blocks:
        codes, power = encode(block)
        message[rows : rows + block.shape[0], :] = codes
        rows += block.shape[0]
        powers.append(power)
    rest = jnp.zeros((8 - len(powers), powers[0].shape[1]), F32)
    message[rows:, :] = jnp.concatenate([*powers, rest])


def read(message, block):
    rows, _ = message.shape
    hidden = (rows - 16) // 3
    codes = message[rows - 16 : rows - 8, :] if block == 3 else message[block * hidden : (block + 1) * hidden, :]
    return decode(codes, message[rows - 8 + block : rows - 7 + block, :])


def prepare_first(kept, sent, came, message, gate):
    rows, _ = kept.shape
    hidden = rows // 3
    parts = [slice(t * hidden, (t + 1) * hidden) for t in range(3)]
    blocks = [kept[part, :] + came[part, :] for part in parts]
    gate[...] = sent[rows:, :] + came[rows:, :]
    write(message, [*blocks, sent[rows:, :] + came[rows:, :]])


def prepare_rest(kept, came, far, plus, minus):
    rows = kept.shape[0] // 2
    hidden = rows // 3
    for i, message in enumerate((plus, minus)):
        parts = [slice(i * rows + t * hidden, i * rows + (t + 1) * hidden) for t in range(3)]
        blocks = [kept[part, :] + came[part, :] for part in parts]
        write(message, blocks + [far[...]])


def count(lines, far_parts, near_parts, own_parts, gate_parts, small):
    line = lax.axis_index("zh")
    shape = small.shape
    lane = lax.broadcasted_iota(jnp.int32, shape, 1)
    row = lax.broadcasted_iota(jnp.int32, shape, 0)
    total = jnp.zeros(shape, F32)

    def put(total, value, where):
        return jnp.where(where, jnp.broadcast_to(value, shape), total)

    def whole(values):
        return jnp.sum(jnp.sum(values, axis=0, keepdims=True), axis=1, keepdims=True)

    for i, step in enumerate((*STEPS, 0)):
        part = (far_parts.at[0], near_parts.at[0], near_parts.at[1], own_parts.at[0])[i]
        expert = 2 * lax.rem(line + step, lines)
        for r in range(2):
            for t in range(3):
                for e in range(2):
                    total = put(total, whole(part[r, t, e]), (row == t) & (lane == r * 8 + expert + e))
    for r in range(2):
        gate_rows = jnp.sum(gate_parts[r], axis=1, keepdims=True)
        for e in range(8):
            total = put(total, gate_rows[e : e + 1, :], (row == 3) & (lane == r * 8 + e))
    small[...] = total


def combine(peers, lines, kept, other, plus, far, minus, message, counted, out, held):
    line, core = lax.axis_index("zh"), lax.axis_index("c")
    rows, width = kept.shape
    hidden = rows // 3
    each = hidden // peers
    factor = 1.0 / (lines * 2 * 2)
    for t in range(3):
        part = pl.ds(t * hidden, hidden)
        soup = kept[part, :] + other[part, :]
        soup = (soup + read(far, t)) + (read(plus, t) + read(minus, t))
        held[part, :] = (soup * factor).astype(jnp.bfloat16).astype(F32)
    gates = [read(ref, 3) for ref in (message, far, plus, minus)]
    serve_gate = (((gates[0] + gates[1]) + (gates[2] + gates[3])) * factor).astype(jnp.bfloat16)
    gate = serve_gate.astype(F32)

    lane = lax.broadcasted_iota(jnp.int32, (4, width), 1)
    row = lax.broadcasted_iota(jnp.int32, (4, width), 0)
    small = counted[...]
    for t in range(3):
        total = jnp.sum(fold(held[t * hidden : (t + 1) * hidden, :]), axis=0, keepdims=True)
        total = jnp.broadcast_to(jnp.sum(total, axis=1, keepdims=True), (4, width))
        small = jnp.where((row == t) & (lane == 16), total, small)
    own_row = lax.broadcasted_iota(jnp.int32, gate.shape, 0) == line * 2 + core
    squares = jnp.sum(jnp.where(own_row, gate * gate, 0.0), axis=0, keepdims=True)
    squares = jnp.broadcast_to(jnp.sum(squares, axis=1, keepdims=True), (4, width))
    small = jnp.where((row == 3) & (lane == 16), squares, small)
    high = small.astype(jnp.bfloat16).astype(F32)
    small = (high + pltpu.roll(small - high, width // 2, 1)).astype(jnp.bfloat16)
    for peer in range(peers):
        out[peer, :8, :] = serve_gate
        for t in range(3):
            start = 8 + t * each
            source = t * hidden + peer * each
            out[peer, start : start + each, :] = held[source : source + each, :].astype(jnp.bfloat16)
        out[peer, 8 + 3 * each :, :] = small


def finish(arrived, out1, out3, out2, gate, soup, replica):
    peers, _, width = arrived.shape
    experts = gate.shape[0]
    each = out1.shape[1]
    for peer in range(peers):
        columns = pl.ds(peer * width, width)
        gate[:, columns] = arrived[peer, :experts, :]
        for k, out in enumerate((out1, out3, out2)):
            start = experts + k * each
            out[0, :, columns] = arrived[peer, start : start + each, :]
    sums = jnp.sum(arrived[:, experts + 3 * each :, :].astype(F32), axis=0)
    sums = sums + pltpu.roll(sums, width // 2, 1)
    lane = lax.broadcasted_iota(jnp.int32, sums.shape, 1)
    row = lax.broadcasted_iota(jnp.int32, sums.shape, 0)
    row_entries = peers * width
    entries = jnp.where(row == 3, row_entries, peers * each * row_entries)
    norms = jnp.sqrt(sums / entries.astype(F32))
    replica[:4, :] = norms[:, :experts]
    replica[4:, :] = pltpu.roll(norms, width - experts, 1)[:, :experts]
    column = jnp.sum(jnp.where(lane == 2 * experts, norms, 0.0), axis=1, keepdims=True)
    soup[...] = jnp.sum(jnp.where(lane == row, column, 0.0), axis=0, keepdims=True)[:, :4]


def steps(rep_w1, rep_w3, rep_w2, rep_gate):
    lines = lax.axis_size("zh")
    peers = lax.axis_size(SA)
    held, experts, hidden, width = rep_w1.shape
    each = hidden // peers
    model_width = width * peers
    rows = 3 * hidden
    swap = [(0, 1), (1, 0)]
    rep_w1, rep_w3, rep_w2, rep_gate = (
        pltpu.with_memory_space_constraint(a, pltpu.HBM) for a in (rep_w1, rep_w3, rep_w2, rep_gate)
    )
    weights = (rep_w1, rep_w3, rep_w2)

    def buffers(n):
        return (pltpu.VMEM((n, 3, held, 2, hidden, width), F32),)

    far_sent, far_kept, far_parts, gate_parts = call(
        functools.partial(local, STEPS[:1], lines),
        (array((rows + 8, width)), array((rows, width)), array((1, held, 3, 2, 8, width)), array((held, 8, width))),
        1 << 22,
        buffers(1)
        + (pltpu.VMEM((held, 8, width), F32), pltpu.SemaphoreType.DMA((1, 3)), pltpu.SemaphoreType.DMA),
        in_hbm=4,
    )(*weights, rep_gate)
    far_came = lax.ppermute(far_sent, "c", swap)
    near_sent, near_kept, near_parts = call(
        functools.partial(local, STEPS[1:], lines),
        (array((2 * rows, width)), array((2 * rows, width)), array((2, held, 3, 2, 8, width))),
        1 << 23,
        buffers(2) + (pltpu.SemaphoreType.DMA((2, 3)),),
        in_hbm=3,
    )(*weights, gate_parts)
    near_came = lax.ppermute(near_sent, "c", swap)
    own_sent, own_kept, own_parts = call(
        functools.partial(local, (0,), lines),
        (array((rows, width)), array((rows, width)), array((1, held, 3, 2, 8, width))),
        1 << 22,
        buffers(1) + (pltpu.SemaphoreType.DMA((1, 3)),),
        in_hbm=3,
    )(*weights, gate_parts)
    own_came = lax.ppermute(own_sent, "c", swap)

    def along(message, step):
        pairs = [(i, (i + step) % lines) for i in range(lines)]
        return lax.ppermute(message.astype(jnp.float16), "zh", pairs).astype(F32)

    half = array((rows + 16, width))
    far, gate = call(prepare_first, (half, array((8, width))), 1 << 20)(far_kept, far_sent, far_came)
    came = {STEPS[0]: along(far, STEPS[0])}
    plus, minus = call(prepare_rest, (half, half), 1 << 21)(
        near_kept, near_came, gate
    )
    came[STEPS[1]] = along(plus, STEPS[1])
    came[STEPS[2]] = along(minus, STEPS[2])
    counted = call(functools.partial(count, lines), array((4, width)), 1 << 20)(
        far_parts, near_parts, own_parts, gate_parts
    )
    message = call(
        functools.partial(combine, peers, lines),
        array((peers, experts + 3 * each + 4, width), jnp.bfloat16),
        1 << 22,
        (pltpu.VMEM((rows, width), F32),),
    )(own_kept, own_came, came[1], came[2], came[3], far.astype(jnp.float16).astype(F32), counted)
    arrived = lax.all_to_all(message, SA, 0, 0, tiled=True)
    shard = array((1, each, model_width), jnp.bfloat16)
    *served, soup_norms, replica_norms = call(
        finish,
        (
            shard,
            shard,
            shard,
            array((experts, model_width), jnp.bfloat16),
            array((1, 4)),
            array((held * 4, experts)),
        ),
        1 << 20,
    )(arrived)
    replica_norms = replica_norms.reshape(held, 4, experts).transpose(0, 2, 1)
    return (*served, soup_norms, replica_norms)


def solution(mesh):
    torus = Mesh(mesh.devices.reshape(mesh.shape["row"] // 2, 2, 2, 4, 4), ROW + SA)
    in_specs = (
        P(ROW, None, None, SA),
        P(ROW, None, None, SA),
        P(ROW, None, None, SA),
        P(ROW, None, SA),
    )
    out_specs = (
        P(ROW, SA, None),
        P(ROW, SA, None),
        P(ROW, SA, None),
        P(),
        P(ROW, None),
        P(ROW, None, None),
    )
    return jax.shard_map(steps, mesh=torus, in_specs=in_specs, out_specs=out_specs, check_vma=False)
```

```python
import functools

import jax
import jax.numpy as jnp
from jax import lax
from jax.experimental import pallas as pl
from jax.experimental.pallas import tpu as pltpu
from jax.sharding import Mesh
from jax.sharding import PartitionSpec as P


ROW = ("zh", "c")
SA = "sa"
FIRST = 26
FULL = 32768.0
LEAST = 2.0**-100
TINY = 2.0**-30
STEPS = (2, 1, 3)
ROOM = 6 << 20
F32 = jnp.float32


def call(kernel, out_shape, flops, scratch=(), in_hbm=0):
    def run(*args):
        specs = [pl.BlockSpec(memory_space=pltpu.HBM)] * in_hbm
        specs += [pl.BlockSpec(memory_space=pltpu.VMEM)] * (len(args) - in_hbm)
        return pl.pallas_call(
            kernel,
            out_shape=out_shape,
            in_specs=specs,
            out_specs=jax.tree.map(lambda _: pl.BlockSpec(memory_space=pltpu.VMEM), out_shape),
            scratch_shapes=scratch,
            compiler_params=pltpu.CompilerParams(vmem_limit_bytes=ROOM),
            cost_estimate=pl.CostEstimate(flops=flops, bytes_accessed=0, transcendentals=0),
        )(*args)

    return run


def array(shape, dtype=F32):
    return jax.ShapeDtypeStruct(shape, dtype)


def fold(values):
    rows, width = values.shape
    return jnp.sum((values * values).reshape(rows // 8, 8, width), axis=0)


def local(steps, lines, *refs):
    weights, refs = refs[:3], refs[3:]
    if steps == STEPS[:1]:
        gate, sent, kept, parts, gate_parts, held, gate_held, done, gate_done = refs
    else:
        _, sent, kept, parts, held, done = refs
    line, core = lax.axis_index("zh"), lax.axis_index("c")
    hidden = held.shape[-2]
    copies = []
    for i, step in enumerate(steps):
        first = 2 * lax.rem(line + step, lines)
        for t, weight in enumerate(weights):
            source = weight.at[:, pl.ds(first, 2)]
            copies.append(pltpu.make_async_copy(source, held.at[i, t], done.at[i, t]))
    if steps == STEPS[:1]:
        gate_copy = pltpu.make_async_copy(gate, gate_held, gate_done)
        gate_copy.start()
    for copy in copies:
        copy.start()
    for i in range(len(steps)):
        for t in range(3):
            copies[3 * i + t].wait()
            rows = pl.ds((3 * i + t) * hidden, hidden)
            sent[rows, :] = held[i, t, 0, 1 - core] + held[i, t, 1, 1 - core]
            kept[rows, :] = held[i, t, 0, core] + held[i, t, 1, core]
            for r in range(2):
                for e in range(2):
                    parts[i, r, t, e] = fold(held[i, t, r, e])
    if steps == STEPS[:1]:
        gate_copy.wait()
        end = 3 * hidden * len(steps)
        sent[end : end + 8, :] = gate_held[0] + gate_held[1]
        gate_parts[...] = gate_held[...] * gate_held[...]


def encode(values):
    top = jnp.max(jnp.abs(values), axis=0, keepdims=True)
    power = jnp.ceil(jnp.log2(jnp.maximum(top, LEAST)))
    parts = values * jnp.exp2(-power)
    return parts * jnp.abs(parts) * FULL, power


def decode(codes, power):
    roots = codes * lax.rsqrt(jnp.maximum(jnp.abs(codes), TINY))
    return roots * (jnp.exp2(power) * (FULL**-0.5))


def write(message, blocks):
    powers = []
    rows = 0
    for block in blocks:
        codes, power = encode(block)
        message[rows : rows + block.shape[0], :] = codes
        rows += block.shape[0]
        powers.append(power)
    rest = jnp.zeros((8 - len(powers), powers[0].shape[1]), F32)
    message[rows:, :] = jnp.concatenate([*powers, rest])


def read(message, block):
    rows, _ = message.shape
    hidden = (rows - 16) // 3
    codes = message[rows - 16 : rows - 8, :] if block == 3 else message[block * hidden : (block + 1) * hidden, :]
    return decode(codes, message[rows - 8 + block : rows - 7 + block, :])


def prepare_first(kept, sent, came, message, gate):
    rows, _ = kept.shape
    hidden = rows // 3
    parts = [slice(t * hidden, (t + 1) * hidden) for t in range(3)]
    blocks = [kept[part, :] + came[part, :] for part in parts]
    gate[...] = sent[rows:, :] + came[rows:, :]
    write(message, [*blocks, sent[rows:, :] + came[rows:, :]])


def prepare_rest(kept, came, far, plus, minus):
    rows = kept.shape[0] // 2
    hidden = rows // 3
    for i, message in enumerate((plus, minus)):
        parts = [slice(i * rows + t * hidden, i * rows + (t + 1) * hidden) for t in range(3)]
        blocks = [kept[part, :] + came[part, :] for part in parts]
        write(message, blocks + [far[...]])


def count(lines, far_parts, near_parts, own_parts, gate_parts, small):
    line = lax.axis_index("zh")
    shape = small.shape
    lane = lax.broadcasted_iota(jnp.int32, shape, 1)
    row = lax.broadcasted_iota(jnp.int32, shape, 0)
    total = jnp.zeros(shape, F32)

    def put(total, value, where):
        return jnp.where(where, jnp.broadcast_to(value, shape), total)

    def whole(values):
        return jnp.sum(jnp.sum(values, axis=0, keepdims=True), axis=1, keepdims=True)

    for i, step in enumerate((*STEPS, 0)):
        part = (far_parts.at[0], near_parts.at[0], near_parts.at[1], own_parts.at[0])[i]
        expert = 2 * lax.rem(line + step, lines)
        for r in range(2):
            for t in range(3):
                for e in range(2):
                    total = put(total, whole(part[r, t, e]), (row == t) & (lane == r * 8 + expert + e))
    for r in range(2):
        gate_rows = jnp.sum(gate_parts[r], axis=1, keepdims=True)
        for e in range(8):
            total = put(total, gate_rows[e : e + 1, :], (row == 3) & (lane == r * 8 + e))
    small[...] = total


def combine(peers, lines, kept, other, plus, far, minus, message, counted, out, held):
    line, core = lax.axis_index("zh"), lax.axis_index("c")
    rows, width = kept.shape
    hidden = rows // 3
    each = hidden // peers
    factor = 1.0 / (lines * 2 * 2)
    for t in range(3):
        part = pl.ds(t * hidden, hidden)
        soup = kept[part, :] + other[part, :]
        soup = (soup + read(far, t)) + (read(plus, t) + read(minus, t))
        held[part, :] = (soup * factor).astype(jnp.bfloat16).astype(F32)
    gates = [read(ref, 3) for ref in (message, far, plus, minus)]
    serve_gate = (((gates[0] + gates[1]) + (gates[2] + gates[3])) * factor).astype(jnp.bfloat16)
    gate = serve_gate.astype(F32)

    lane = lax.broadcasted_iota(jnp.int32, (4, width), 1)
    row = lax.broadcasted_iota(jnp.int32, (4, width), 0)
    small = counted[...]
    for t in range(3):
        total = jnp.sum(fold(held[t * hidden : (t + 1) * hidden, :]), axis=0, keepdims=True)
        total = jnp.broadcast_to(jnp.sum(total, axis=1, keepdims=True), (4, width))
        small = jnp.where((row == t) & (lane == 16), total, small)
    own_row = lax.broadcasted_iota(jnp.int32, gate.shape, 0) == line * 2 + core
    squares = jnp.sum(jnp.where(own_row, gate * gate, 0.0), axis=0, keepdims=True)
    squares = jnp.broadcast_to(jnp.sum(squares, axis=1, keepdims=True), (4, width))
    small = jnp.where((row == 3) & (lane == 16), squares, small)
    high = small.astype(jnp.bfloat16).astype(F32)
    small = (high + pltpu.roll(small - high, width // 2, 1)).astype(jnp.bfloat16)
    for peer in range(peers):
        out[peer, :8, :] = serve_gate
        for t in range(3):
            start = 8 + t * each
            source = t * hidden + (peer ^ FIRST) * each
            out[peer, start : start + each, :] = held[source : source + each, :].astype(jnp.bfloat16)
        out[peer, 8 + 3 * each :, :] = small


def finish(arrived, out1, out3, out2, gate, soup, replica):
    peers, _, width = arrived.shape
    experts = gate.shape[0]
    each = out1.shape[1]
    for peer in range(peers):
        columns = pl.ds((peer ^ FIRST) * width, width)
        gate[:, columns] = arrived[peer, :experts, :]
        for k, out in enumerate((out1, out3, out2)):
            start = experts + k * each
            out[0, :, columns] = arrived[peer, start : start + each, :]
    sums = jnp.sum(arrived[:, experts + 3 * each :, :].astype(F32), axis=0)
    sums = sums + pltpu.roll(sums, width // 2, 1)
    lane = lax.broadcasted_iota(jnp.int32, sums.shape, 1)
    row = lax.broadcasted_iota(jnp.int32, sums.shape, 0)
    row_entries = peers * width
    entries = jnp.where(row == 3, row_entries, peers * each * row_entries)
    norms = jnp.sqrt(sums / entries.astype(F32))
    replica[:4, :] = norms[:, :experts]
    replica[4:, :] = pltpu.roll(norms, width - experts, 1)[:, :experts]
    column = jnp.sum(jnp.where(lane == 2 * experts, norms, 0.0), axis=1, keepdims=True)
    soup[...] = jnp.sum(jnp.where(lane == row, column, 0.0), axis=0, keepdims=True)[:, :4]


def steps(rep_w1, rep_w3, rep_w2, rep_gate):
    lines = lax.axis_size("zh")
    peers = lax.axis_size(SA)
    held, experts, hidden, width = rep_w1.shape
    each = hidden // peers
    model_width = width * peers
    rows = 3 * hidden
    swap = [(0, 1), (1, 0)]
    rep_w1, rep_w3, rep_w2, rep_gate = (
        pltpu.with_memory_space_constraint(a, pltpu.HBM) for a in (rep_w1, rep_w3, rep_w2, rep_gate)
    )
    weights = (rep_w1, rep_w3, rep_w2)

    def buffers(n):
        return (pltpu.VMEM((n, 3, held, 2, hidden, width), F32),)

    far_sent, far_kept, far_parts, gate_parts = call(
        functools.partial(local, STEPS[:1], lines),
        (array((rows + 8, width)), array((rows, width)), array((1, held, 3, 2, 8, width)), array((held, 8, width))),
        1 << 22,
        buffers(1)
        + (pltpu.VMEM((held, 8, width), F32), pltpu.SemaphoreType.DMA((1, 3)), pltpu.SemaphoreType.DMA),
        in_hbm=4,
    )(*weights, rep_gate)
    far_came = lax.ppermute(far_sent, "c", swap)
    near_sent, near_kept, near_parts = call(
        functools.partial(local, STEPS[1:], lines),
        (array((2 * rows, width)), array((2 * rows, width)), array((2, held, 3, 2, 8, width))),
        1 << 23,
        buffers(2) + (pltpu.SemaphoreType.DMA((2, 3)),),
        in_hbm=3,
    )(*weights, gate_parts)
    near_came = lax.ppermute(near_sent, "c", swap)
    own_sent, own_kept, own_parts = call(
        functools.partial(local, (0,), lines),
        (array((rows, width)), array((rows, width)), array((1, held, 3, 2, 8, width))),
        1 << 22,
        buffers(1) + (pltpu.SemaphoreType.DMA((1, 3)),),
        in_hbm=3,
    )(*weights, gate_parts)
    own_came = lax.ppermute(own_sent, "c", swap)

    def along(message, step):
        pairs = [(i, (i + step) % lines) for i in range(lines)]
        return lax.ppermute(message.astype(jnp.float16), "zh", pairs).astype(F32)

    half = array((rows + 16, width))
    far, gate = call(prepare_first, (half, array((8, width))), 1 << 20)(far_kept, far_sent, far_came)
    came = {STEPS[0]: along(far, STEPS[0])}
    plus, minus = call(prepare_rest, (half, half), 1 << 21)(
        near_kept, near_came, gate
    )
    came[STEPS[1]] = along(plus, STEPS[1])
    came[STEPS[2]] = along(minus, STEPS[2])
    counted = call(functools.partial(count, lines), array((4, width)), 1 << 20)(
        far_parts, near_parts, own_parts, gate_parts
    )
    message = call(
        functools.partial(combine, peers, lines),
        array((peers, experts + 3 * each + 4, width), jnp.bfloat16),
        1 << 22,
        (pltpu.VMEM((rows, width), F32),),
    )(own_kept, own_came, came[1], came[2], came[3], far.astype(jnp.float16).astype(F32), counted)
    arrived = lax.all_to_all(
        message, SA, 0, 0, axis_index_groups=[[peer ^ FIRST for peer in range(peers)]], tiled=True
    )
    shard = array((1, each, model_width), jnp.bfloat16)
    *served, soup_norms, replica_norms = call(
        finish,
        (
            shard,
            shard,
            shard,
            array((experts, model_width), jnp.bfloat16),
            array((1, 4)),
            array((held * 4, experts)),
        ),
        1 << 20,
    )(arrived)
    replica_norms = replica_norms.reshape(held, 4, experts).transpose(0, 2, 1)
    return (*served, soup_norms, replica_norms)


def solution(mesh):
    torus = Mesh(mesh.devices.reshape(mesh.shape["row"] // 2, 2, -1), (*ROW, SA))
    in_specs = (
        P(ROW, None, None, SA),
        P(ROW, None, None, SA),
        P(ROW, None, None, SA),
        P(ROW, None, SA),
    )
    out_specs = (
        P(ROW, SA, None),
        P(ROW, SA, None),
        P(ROW, SA, None),
        P(),
        P(ROW, None),
        P(ROW, None, None),
    )
    return jax.shard_map(steps, mesh=torus, in_specs=in_specs, out_specs=out_specs, check_vma=False)
```

```python
import functools

import jax
import jax.numpy as jnp
from jax import lax
from jax.experimental import pallas as pl
from jax.experimental.pallas import tpu as pltpu
from jax.sharding import Mesh
from jax.sharding import PartitionSpec as P


ROW = ("zh", "c")
SA = "sa"
FIRST = 26
FULL = 32768.0
LEAST = 2.0**-100
TINY = 2.0**-30
STEPS = (1, 2, 3)
TO = ((0, 1, 2, 3), (3, 2, 0, 1), (1, 0, 3, 2), (2, 3, 1, 0))


def partner(line, step):
    return sum(jnp.where(line == k, to, 0) for k, to in enumerate(TO[step]))


ROOM = 6 << 20
F32 = jnp.float32


def call(kernel, out_shape, flops, scratch=(), in_hbm=0):
    def run(*args):
        specs = [pl.BlockSpec(memory_space=pltpu.HBM)] * in_hbm
        specs += [pl.BlockSpec(memory_space=pltpu.VMEM)] * (len(args) - in_hbm)
        return pl.pallas_call(
            kernel,
            out_shape=out_shape,
            in_specs=specs,
            out_specs=jax.tree.map(lambda _: pl.BlockSpec(memory_space=pltpu.VMEM), out_shape),
            scratch_shapes=scratch,
            compiler_params=pltpu.CompilerParams(vmem_limit_bytes=ROOM),
            cost_estimate=pl.CostEstimate(flops=flops, bytes_accessed=0, transcendentals=0),
        )(*args)

    return run


def array(shape, dtype=F32):
    return jax.ShapeDtypeStruct(shape, dtype)


def fold(values):
    rows, width = values.shape
    return jnp.sum((values * values).reshape(rows // 8, 8, width), axis=0)


def local(steps, *refs):
    weights, refs = refs[:3], refs[3:]
    if steps == STEPS[:1]:
        gate, sent, kept, parts, gate_parts, held, gate_held, done, gate_done = refs
    else:
        _, sent, kept, parts, held, done = refs
    line, core = lax.axis_index("zh"), lax.axis_index("c")
    hidden = held.shape[-2]
    copies = []
    for i, step in enumerate(steps):
        first = 2 * partner(line, step)
        for t, weight in enumerate(weights):
            source = weight.at[:, pl.ds(first, 2)]
            copies.append(pltpu.make_async_copy(source, held.at[i, t], done.at[i, t]))
    if steps == STEPS[:1]:
        gate_copy = pltpu.make_async_copy(gate, gate_held, gate_done)
        gate_copy.start()
    for copy in copies:
        copy.start()
    for i in range(len(steps)):
        for t in range(3):
            copies[3 * i + t].wait()
            rows = pl.ds((3 * i + t) * hidden, hidden)
            sent[rows, :] = held[i, t, 0, 1 - core] + held[i, t, 1, 1 - core]
            kept[rows, :] = held[i, t, 0, core] + held[i, t, 1, core]
            for r in range(2):
                for e in range(2):
                    parts[i, r, t, e] = fold(held[i, t, r, e])
    if steps == STEPS[:1]:
        gate_copy.wait()
        end = 3 * hidden * len(steps)
        sent[end : end + 8, :] = gate_held[0] + gate_held[1]
        gate_parts[...] = gate_held[...] * gate_held[...]


def encode(values):
    top = jnp.max(jnp.abs(values), axis=0, keepdims=True)
    power = jnp.ceil(jnp.log2(jnp.maximum(top, LEAST)))
    parts = values * jnp.exp2(-power)
    return parts * jnp.abs(parts) * FULL, power


def decode(codes, power):
    roots = codes * lax.rsqrt(jnp.maximum(jnp.abs(codes), TINY))
    return roots * (jnp.exp2(power) * (FULL**-0.5))


def write(message, blocks):
    powers = []
    rows = 0
    for block in blocks:
        codes, power = encode(block)
        message[rows : rows + block.shape[0], :] = codes
        rows += block.shape[0]
        powers.append(power)
    rest = jnp.zeros((8 - len(powers), powers[0].shape[1]), F32)
    message[rows:, :] = jnp.concatenate([*powers, rest])


def read(message, block):
    rows, _ = message.shape
    hidden = (rows - 16) // 3
    codes = message[rows - 16 : rows - 8, :] if block == 3 else message[block * hidden : (block + 1) * hidden, :]
    return decode(codes, message[rows - 8 + block : rows - 7 + block, :])


def prepare_first(kept, sent, came, message, gate):
    rows, _ = kept.shape
    hidden = rows // 3
    parts = [slice(t * hidden, (t + 1) * hidden) for t in range(3)]
    blocks = [kept[part, :] + came[part, :] for part in parts]
    gate[...] = sent[rows:, :] + came[rows:, :]
    write(message, [*blocks, sent[rows:, :] + came[rows:, :]])


def prepare_rest(kept, came, far, plus, minus):
    rows = kept.shape[0] // 2
    hidden = rows // 3
    for i, message in enumerate((plus, minus)):
        parts = [slice(i * rows + t * hidden, i * rows + (t + 1) * hidden) for t in range(3)]
        blocks = [kept[part, :] + came[part, :] for part in parts]
        write(message, blocks + [far[...]])


def count(far_parts, near_parts, own_parts, gate_parts, small):
    line = lax.axis_index("zh")
    shape = small.shape
    lane = lax.broadcasted_iota(jnp.int32, shape, 1)
    row = lax.broadcasted_iota(jnp.int32, shape, 0)
    total = jnp.zeros(shape, F32)

    def put(total, value, where):
        return jnp.where(where, jnp.broadcast_to(value, shape), total)

    def whole(values):
        return jnp.sum(jnp.sum(values, axis=0, keepdims=True), axis=1, keepdims=True)

    for i, step in enumerate((*STEPS, 0)):
        part = (far_parts.at[0], near_parts.at[0], near_parts.at[1], own_parts.at[0])[i]
        expert = 2 * partner(line, step)
        for r in range(2):
            for t in range(3):
                for e in range(2):
                    total = put(total, whole(part[r, t, e]), (row == t) & (lane == r * 8 + expert + e))
    for r in range(2):
        gate_rows = jnp.sum(gate_parts[r], axis=1, keepdims=True)
        for e in range(8):
            total = put(total, gate_rows[e : e + 1, :], (row == 3) & (lane == r * 8 + e))
    small[...] = total


def combine(peers, lines, kept, other, plus, far, minus, message, counted, out, held):
    line, core = lax.axis_index("zh"), lax.axis_index("c")
    rows, width = kept.shape
    hidden = rows // 3
    each = hidden // peers
    factor = 1.0 / (lines * 2 * 2)
    for t in range(3):
        part = pl.ds(t * hidden, hidden)
        soup = kept[part, :] + other[part, :]
        soup = (soup + read(far, t)) + (read(plus, t) + read(minus, t))
        held[part, :] = (soup * factor).astype(jnp.bfloat16).astype(F32)
    gates = [read(ref, 3) for ref in (message, far, plus, minus)]
    serve_gate = (((gates[0] + gates[1]) + (gates[2] + gates[3])) * factor).astype(jnp.bfloat16)
    gate = serve_gate.astype(F32)

    lane = lax.broadcasted_iota(jnp.int32, (4, width), 1)
    row = lax.broadcasted_iota(jnp.int32, (4, width), 0)
    small = counted[...]
    for t in range(3):
        total = jnp.sum(fold(held[t * hidden : (t + 1) * hidden, :]), axis=0, keepdims=True)
        total = jnp.broadcast_to(jnp.sum(total, axis=1, keepdims=True), (4, width))
        small = jnp.where((row == t) & (lane == 16), total, small)
    own_row = lax.broadcasted_iota(jnp.int32, gate.shape, 0) == line * 2 + core
    squares = jnp.sum(jnp.where(own_row, gate * gate, 0.0), axis=0, keepdims=True)
    squares = jnp.broadcast_to(jnp.sum(squares, axis=1, keepdims=True), (4, width))
    small = jnp.where((row == 3) & (lane == 16), squares, small)
    high = small.astype(jnp.bfloat16).astype(F32)
    small = (high + pltpu.roll(small - high, width // 2, 1)).astype(jnp.bfloat16)
    for peer in range(peers):
        out[peer, :8, :] = serve_gate
        for t in range(3):
            start = 8 + t * each
            source = t * hidden + (peer ^ FIRST) * each
            out[peer, start : start + each, :] = held[source : source + each, :].astype(jnp.bfloat16)
        out[peer, 8 + 3 * each :, :] = small


def finish(arrived, out1, out3, out2, gate, soup, replica):
    peers, _, width = arrived.shape
    experts = gate.shape[0]
    each = out1.shape[1]
    for peer in range(peers):
        columns = pl.ds((peer ^ FIRST) * width, width)
        gate[:, columns] = arrived[peer, :experts, :]
        for k, out in enumerate((out1, out3, out2)):
            start = experts + k * each
            out[0, :, columns] = arrived[peer, start : start + each, :]
    sums = jnp.sum(arrived[:, experts + 3 * each :, :].astype(F32), axis=0)
    sums = sums + pltpu.roll(sums, width // 2, 1)
    lane = lax.broadcasted_iota(jnp.int32, sums.shape, 1)
    row = lax.broadcasted_iota(jnp.int32, sums.shape, 0)
    row_entries = peers * width
    entries = jnp.where(row == 3, row_entries, peers * each * row_entries)
    norms = jnp.sqrt(sums / entries.astype(F32))
    replica[:4, :] = norms[:, :experts]
    replica[4:, :] = pltpu.roll(norms, width - experts, 1)[:, :experts]
    column = jnp.sum(jnp.where(lane == 2 * experts, norms, 0.0), axis=1, keepdims=True)
    soup[...] = jnp.sum(jnp.where(lane == row, column, 0.0), axis=0, keepdims=True)[:, :4]


def steps(rep_w1, rep_w3, rep_w2, rep_gate):
    lines = lax.axis_size("zh")
    peers = lax.axis_size(SA)
    held, experts, hidden, width = rep_w1.shape
    each = hidden // peers
    model_width = width * peers
    rows = 3 * hidden
    swap = [(0, 1), (1, 0)]
    rep_w1, rep_w3, rep_w2, rep_gate = (
        pltpu.with_memory_space_constraint(a, pltpu.HBM) for a in (rep_w1, rep_w3, rep_w2, rep_gate)
    )
    weights = (rep_w1, rep_w3, rep_w2)

    def buffers(n):
        return (pltpu.VMEM((n, 3, held, 2, hidden, width), F32),)

    far_sent, far_kept, far_parts, gate_parts = call(
        functools.partial(local, STEPS[:1]),
        (array((rows + 8, width)), array((rows, width)), array((1, held, 3, 2, 8, width)), array((held, 8, width))),
        1 << 22,
        buffers(1)
        + (pltpu.VMEM((held, 8, width), F32), pltpu.SemaphoreType.DMA((1, 3)), pltpu.SemaphoreType.DMA),
        in_hbm=4,
    )(*weights, rep_gate)
    far_came = lax.ppermute(far_sent, "c", swap)
    near_sent, near_kept, near_parts = call(
        functools.partial(local, STEPS[1:]),
        (array((2 * rows, width)), array((2 * rows, width)), array((2, held, 3, 2, 8, width))),
        1 << 23,
        buffers(2) + (pltpu.SemaphoreType.DMA((2, 3)),),
        in_hbm=3,
    )(*weights, gate_parts)
    near_came = lax.ppermute(near_sent, "c", swap)
    own_sent, own_kept, own_parts = call(
        functools.partial(local, (0,)),
        (array((rows, width)), array((rows, width)), array((1, held, 3, 2, 8, width))),
        1 << 22,
        buffers(1) + (pltpu.SemaphoreType.DMA((1, 3)),),
        in_hbm=3,
    )(*weights, gate_parts)
    own_came = lax.ppermute(own_sent, "c", swap)

    def along(message, step):
        pairs = list(enumerate(TO[step]))
        return lax.ppermute(message.astype(jnp.float16), "zh", pairs).astype(F32)

    half = array((rows + 16, width))
    far, gate = call(prepare_first, (half, array((8, width))), 1 << 20)(far_kept, far_sent, far_came)
    came = {STEPS[0]: along(far, STEPS[0])}
    plus, minus = call(prepare_rest, (half, half), 1 << 21)(
        near_kept, near_came, gate
    )
    came[STEPS[1]] = along(plus, STEPS[1])
    came[STEPS[2]] = along(minus, STEPS[2])
    counted = call(count, array((4, width)), 1 << 20)(far_parts, near_parts, own_parts, gate_parts)
    message = call(
        functools.partial(combine, peers, lines),
        array((peers, experts + 3 * each + 4, width), jnp.bfloat16),
        1 << 22,
        (pltpu.VMEM((rows, width), F32),),
    )(own_kept, own_came, came[1], came[2], came[3], far.astype(jnp.float16).astype(F32), counted)
    arrived = lax.all_to_all(
        message, SA, 0, 0, axis_index_groups=[[peer ^ FIRST for peer in range(peers)]], tiled=True
    )
    shard = array((1, each, model_width), jnp.bfloat16)
    *served, soup_norms, replica_norms = call(
        finish,
        (
            shard,
            shard,
            shard,
            array((experts, model_width), jnp.bfloat16),
            array((1, 4)),
            array((held * 4, experts)),
        ),
        1 << 20,
    )(arrived)
    replica_norms = replica_norms.reshape(held, 4, experts).transpose(0, 2, 1)
    return (*served, soup_norms, replica_norms)


def solution(mesh):
    torus = Mesh(mesh.devices.reshape(mesh.shape["row"] // 2, 2, -1), (*ROW, SA))
    in_specs = (
        P(ROW, None, None, SA),
        P(ROW, None, None, SA),
        P(ROW, None, None, SA),
        P(ROW, None, SA),
    )
    out_specs = (
        P(ROW, SA, None),
        P(ROW, SA, None),
        P(ROW, SA, None),
        P(),
        P(ROW, None),
        P(ROW, None, None),
    )
    return jax.shard_map(steps, mesh=torus, in_specs=in_specs, out_specs=out_specs, check_vma=False)
```

```python
import functools

import jax
import jax.numpy as jnp
from jax import lax
from jax.experimental import pallas as pl
from jax.experimental.pallas import tpu as pltpu
from jax.sharding import Mesh
from jax.sharding import PartitionSpec as P


ROW = ("zh", "c")
SA = "sa"
FIRST = 26
FULL = 32768.0
LEAST = 2.0**-100
TINY = 2.0**-30
STEPS = (1, 2, 3)
TO = ((0, 1, 2, 3), (3, 2, 0, 1), (1, 0, 3, 2), (2, 3, 1, 0))


def partner(line, step):
    return sum(jnp.where(line == k, to, 0) for k, to in enumerate(TO[step]))


ROOM = 6 << 20
F32 = jnp.float32


def call(kernel, out_shape, flops, scratch=(), in_hbm=0):
    def run(*args):
        specs = [pl.BlockSpec(memory_space=pltpu.HBM)] * in_hbm
        specs += [pl.BlockSpec(memory_space=pltpu.VMEM)] * (len(args) - in_hbm)
        return pl.pallas_call(
            kernel,
            out_shape=out_shape,
            in_specs=specs,
            out_specs=jax.tree.map(lambda _: pl.BlockSpec(memory_space=pltpu.VMEM), out_shape),
            scratch_shapes=scratch,
            compiler_params=pltpu.CompilerParams(vmem_limit_bytes=ROOM),
            cost_estimate=pl.CostEstimate(flops=flops, bytes_accessed=0, transcendentals=0),
        )(*args)

    return run


def array(shape, dtype=F32):
    return jax.ShapeDtypeStruct(shape, dtype)


def fold(values):
    rows, width = values.shape
    return jnp.sum((values * values).reshape(rows // 8, 8, width), axis=0)


def local(steps, *refs):
    weights, refs = refs[:3], refs[3:]
    if steps == STEPS[:1]:
        gate, sent, kept, parts, gate_parts, held, gate_held, done, gate_done = refs
    else:
        _, sent, kept, parts, held, done = refs
    line, core = lax.axis_index("zh"), lax.axis_index("c")
    hidden = held.shape[-2]
    copies = []
    for i, step in enumerate(steps):
        first = 2 * partner(line, step)
        for t, weight in enumerate(weights):
            source = weight.at[:, pl.ds(first, 2)]
            copies.append(pltpu.make_async_copy(source, held.at[i, t], done.at[i, t]))
    if steps == STEPS[:1]:
        gate_copy = pltpu.make_async_copy(gate, gate_held, gate_done)
        gate_copy.start()
    for copy in copies:
        copy.start()
    for i in range(len(steps)):
        for t in range(3):
            copies[3 * i + t].wait()
            rows = pl.ds((3 * i + t) * hidden, hidden)
            sent[rows, :] = held[i, t, 0, 1 - core] + held[i, t, 1, 1 - core]
            kept[rows, :] = held[i, t, 0, core] + held[i, t, 1, core]
            for r in range(2):
                for e in range(2):
                    parts[i, r, t, e] = fold(held[i, t, r, e])
    if steps == STEPS[:1]:
        gate_copy.wait()
        end = 3 * hidden * len(steps)
        sent[end : end + 8, :] = gate_held[0] + gate_held[1]
        gate_parts[...] = gate_held[...] * gate_held[...]


def encode(values):
    top = jnp.max(jnp.abs(values), axis=0, keepdims=True)
    power = jnp.ceil(jnp.log2(jnp.maximum(top, LEAST)))
    parts = values * jnp.exp2(-power)
    return parts * jnp.abs(parts) * FULL, power


def decode(codes, power):
    roots = codes * lax.rsqrt(jnp.maximum(jnp.abs(codes), TINY))
    return roots * (jnp.exp2(power) * (FULL**-0.5))


def write(message, blocks):
    powers = []
    rows = 0
    for block in blocks:
        codes, power = encode(block)
        message[rows : rows + block.shape[0], :] = codes
        rows += block.shape[0]
        powers.append(power)
    rest = jnp.zeros((8 - len(powers), powers[0].shape[1]), F32)
    message[rows:, :] = jnp.concatenate([*powers, rest])


def read(message, block):
    rows, _ = message.shape
    hidden = (rows - 16) // 3
    codes = message[rows - 16 : rows - 8, :] if block == 3 else message[block * hidden : (block + 1) * hidden, :]
    return decode(codes, message[rows - 8 + block : rows - 7 + block, :])


def prepare_first(kept, sent, came, message, gate):
    rows, _ = kept.shape
    hidden = rows // 3
    parts = [slice(t * hidden, (t + 1) * hidden) for t in range(3)]
    blocks = [kept[part, :] + came[part, :] for part in parts]
    gate[...] = sent[rows:, :] + came[rows:, :]
    write(message, [*blocks, sent[rows:, :] + came[rows:, :]])


def prepare_rest(kept, came, far, plus, minus):
    rows = kept.shape[0] // 2
    hidden = rows // 3
    for i, message in enumerate((plus, minus)):
        parts = [slice(i * rows + t * hidden, i * rows + (t + 1) * hidden) for t in range(3)]
        blocks = [kept[part, :] + came[part, :] for part in parts]
        write(message, blocks + [far[...]])


def count(far_parts, near_parts, own_parts, gate_parts, small):
    line = lax.axis_index("zh")
    shape = small.shape
    lane = lax.broadcasted_iota(jnp.int32, shape, 1)
    row = lax.broadcasted_iota(jnp.int32, shape, 0)
    total = jnp.zeros(shape, F32)

    def put(total, value, where):
        return jnp.where(where, jnp.broadcast_to(value, shape), total)

    def whole(values):
        return jnp.sum(jnp.sum(values, axis=0, keepdims=True), axis=1, keepdims=True)

    for i, step in enumerate((*STEPS, 0)):
        part = (far_parts.at[0], near_parts.at[0], near_parts.at[1], own_parts.at[0])[i]
        expert = 2 * partner(line, step)
        for r in range(2):
            for t in range(3):
                for e in range(2):
                    total = put(total, whole(part[r, t, e]), (row == t) & (lane == r * 8 + expert + e))
    for r in range(2):
        gate_rows = jnp.sum(gate_parts[r], axis=1, keepdims=True)
        for e in range(8):
            total = put(total, gate_rows[e : e + 1, :], (row == 3) & (lane == r * 8 + e))
    small[...] = total


def decode_first(message, values):
    rows = message.shape[0]
    hidden = (rows - 16) // 3
    for t in range(3):
        values[t * hidden : (t + 1) * hidden, :] = read(message, t)
    values[rows - 16 :, :] = message[rows - 16 :, :]


def combine(peers, lines, kept, other, plus, far, minus, message, counted, out, held):
    line, core = lax.axis_index("zh"), lax.axis_index("c")
    rows, width = kept.shape
    hidden = rows // 3
    each = hidden // peers
    factor = 1.0 / (lines * 2 * 2)
    for t in range(3):
        part = pl.ds(t * hidden, hidden)
        soup = kept[part, :] + other[part, :]
        soup = (soup + read(far, t)) + (plus[part, :] + read(minus, t))
        held[part, :] = (soup * factor).astype(jnp.bfloat16).astype(F32)
    gates = [read(ref, 3) for ref in (message, far, plus, minus)]
    serve_gate = (((gates[0] + gates[1]) + (gates[2] + gates[3])) * factor).astype(jnp.bfloat16)
    gate = serve_gate.astype(F32)

    lane = lax.broadcasted_iota(jnp.int32, (4, width), 1)
    row = lax.broadcasted_iota(jnp.int32, (4, width), 0)
    small = counted[...]
    for t in range(3):
        total = jnp.sum(fold(held[t * hidden : (t + 1) * hidden, :]), axis=0, keepdims=True)
        total = jnp.broadcast_to(jnp.sum(total, axis=1, keepdims=True), (4, width))
        small = jnp.where((row == t) & (lane == 16), total, small)
    own_row = lax.broadcasted_iota(jnp.int32, gate.shape, 0) == line * 2 + core
    squares = jnp.sum(jnp.where(own_row, gate * gate, 0.0), axis=0, keepdims=True)
    squares = jnp.broadcast_to(jnp.sum(squares, axis=1, keepdims=True), (4, width))
    small = jnp.where((row == 3) & (lane == 16), squares, small)
    high = small.astype(jnp.bfloat16).astype(F32)
    small = (high + pltpu.roll(small - high, width // 2, 1)).astype(jnp.bfloat16)
    for peer in range(peers):
        out[peer, :8, :] = serve_gate
        for t in range(3):
            start = 8 + t * each
            source = t * hidden + (peer ^ FIRST) * each
            out[peer, start : start + each, :] = held[source : source + each, :].astype(jnp.bfloat16)
        out[peer, 8 + 3 * each :, :] = small


def finish(arrived, out1, out3, out2, gate, soup, replica):
    peers, _, width = arrived.shape
    experts = gate.shape[0]
    each = out1.shape[1]
    for peer in range(peers):
        columns = pl.ds((peer ^ FIRST) * width, width)
        gate[:, columns] = arrived[peer, :experts, :]
        for k, out in enumerate((out1, out3, out2)):
            start = experts + k * each
            out[0, :, columns] = arrived[peer, start : start + each, :]
    sums = jnp.sum(arrived[:, experts + 3 * each :, :].astype(F32), axis=0)
    sums = sums + pltpu.roll(sums, width // 2, 1)
    lane = lax.broadcasted_iota(jnp.int32, sums.shape, 1)
    row = lax.broadcasted_iota(jnp.int32, sums.shape, 0)
    row_entries = peers * width
    entries = jnp.where(row == 3, row_entries, peers * each * row_entries)
    norms = jnp.sqrt(sums / entries.astype(F32))
    replica[:4, :] = norms[:, :experts]
    replica[4:, :] = pltpu.roll(norms, width - experts, 1)[:, :experts]
    column = jnp.sum(jnp.where(lane == 2 * experts, norms, 0.0), axis=1, keepdims=True)
    soup[...] = jnp.sum(jnp.where(lane == row, column, 0.0), axis=0, keepdims=True)[:, :4]


def steps(rep_w1, rep_w3, rep_w2, rep_gate):
    lines = lax.axis_size("zh")
    peers = lax.axis_size(SA)
    held, experts, hidden, width = rep_w1.shape
    each = hidden // peers
    model_width = width * peers
    rows = 3 * hidden
    swap = [(0, 1), (1, 0)]
    rep_w1, rep_w3, rep_w2, rep_gate = (
        pltpu.with_memory_space_constraint(a, pltpu.HBM) for a in (rep_w1, rep_w3, rep_w2, rep_gate)
    )
    weights = (rep_w1, rep_w3, rep_w2)

    def buffers(n):
        return (pltpu.VMEM((n, 3, held, 2, hidden, width), F32),)

    far_sent, far_kept, far_parts, gate_parts = call(
        functools.partial(local, STEPS[:1]),
        (array((rows + 8, width)), array((rows, width)), array((1, held, 3, 2, 8, width)), array((held, 8, width))),
        1 << 22,
        buffers(1)
        + (pltpu.VMEM((held, 8, width), F32), pltpu.SemaphoreType.DMA((1, 3)), pltpu.SemaphoreType.DMA),
        in_hbm=4,
    )(*weights, rep_gate)
    far_came = lax.ppermute(far_sent, "c", swap)
    near_sent, near_kept, near_parts = call(
        functools.partial(local, STEPS[1:]),
        (array((2 * rows, width)), array((2 * rows, width)), array((2, held, 3, 2, 8, width))),
        1 << 23,
        buffers(2) + (pltpu.SemaphoreType.DMA((2, 3)),),
        in_hbm=3,
    )(*weights, gate_parts)
    near_came = lax.ppermute(near_sent, "c", swap)
    own_sent, own_kept, own_parts = call(
        functools.partial(local, (0,)),
        (array((rows, width)), array((rows, width)), array((1, held, 3, 2, 8, width))),
        1 << 22,
        buffers(1) + (pltpu.SemaphoreType.DMA((1, 3)),),
        in_hbm=3,
    )(*weights, gate_parts)
    own_came = lax.ppermute(own_sent, "c", swap)

    def along(message, step):
        pairs = list(enumerate(TO[step]))
        return lax.ppermute(message.astype(jnp.float16), "zh", pairs).astype(F32)

    half = array((rows + 16, width))
    far, gate = call(prepare_first, (half, array((8, width))), 1 << 20)(far_kept, far_sent, far_came)
    came = {STEPS[0]: along(far, STEPS[0])}
    plus, minus = call(prepare_rest, (half, half), 1 << 21)(
        near_kept, near_came, gate
    )
    came[STEPS[1]] = along(plus, STEPS[1])
    came[STEPS[2]] = along(minus, STEPS[2])
    counted = call(count, array((4, width)), 1 << 20)(far_parts, near_parts, own_parts, gate_parts)
    early = call(decode_first, array((rows + 16, width)), 1 << 20)(came[1])
    message = call(
        functools.partial(combine, peers, lines),
        array((peers, experts + 3 * each + 4, width), jnp.bfloat16),
        1 << 22,
        (pltpu.VMEM((rows, width), F32),),
    )(own_kept, own_came, early, came[2], came[3], far.astype(jnp.float16).astype(F32), counted)
    arrived = lax.all_to_all(
        message, SA, 0, 0, axis_index_groups=[[peer ^ FIRST for peer in range(peers)]], tiled=True
    )
    shard = array((1, each, model_width), jnp.bfloat16)
    *served, soup_norms, replica_norms = call(
        finish,
        (
            shard,
            shard,
            shard,
            array((experts, model_width), jnp.bfloat16),
            array((1, 4)),
            array((held * 4, experts)),
        ),
        1 << 20,
    )(arrived)
    replica_norms = replica_norms.reshape(held, 4, experts).transpose(0, 2, 1)
    return (*served, soup_norms, replica_norms)


def solution(mesh):
    torus = Mesh(mesh.devices.reshape(mesh.shape["row"] // 2, 2, -1), (*ROW, SA))
    in_specs = (
        P(ROW, None, None, SA),
        P(ROW, None, None, SA),
        P(ROW, None, None, SA),
        P(ROW, None, SA),
    )
    out_specs = (
        P(ROW, SA, None),
        P(ROW, SA, None),
        P(ROW, SA, None),
        P(),
        P(ROW, None),
        P(ROW, None, None),
    )
    return jax.shard_map(steps, mesh=torus, in_specs=in_specs, out_specs=out_specs, check_vma=False)
```
